8 devices in a mesh: dp: 1 (over z), sp: 8 (over x, y, core).
Axes of the slice: x: 2, y: 2, z: 1, core: 2. Of those that a mesh axis runs over, the one named last changes fastest.
Arguments:
- x: bfloat16 [4096, 3072], P(('dp', 'sp'))
- gain: bfloat16 [3072], replicated
- wq: bfloat16 [3072, 3072], P('sp')
- wk: bfloat16 [3072, 1024], P('sp')
- wv: bfloat16 [3072, 1024], P('sp')
- wo: bfloat16 [3072, 3072], P('sp')
Outputs:
- output: bfloat16 [4096, 3072], P(('dp', 'sp'))
All inputs are finite; a program needn't handle non-finite values.
Results may differ from the reference program's by a relative error of at most 0.012.
Values are sent between devices in bfloat16 or wider.
A program may use at most 2 GiB of HBM per device.

```python
import jax
import jax.numpy as jnp
from jax import lax

ROWS = 4096
D = 3072
HEADS = 24
KV_HEADS = 8
HEAD = 128
THETA = 10000


def setup_inputs(seed: int = 0, part: int = 0) -> dict:
    kx, kn, kq, kk, kv, ko = jax.random.split(jax.random.key(seed), 6)

    def weights(key, rows, columns):
        return jax.random.normal(key, (rows, columns), jnp.float32) * rows**-0.5

    drawn = {
        "x": jax.random.normal(jax.random.fold_in(kx, part), (ROWS, D), jnp.float32),
        "gain": 1 + 0.1 * jax.random.normal(kn, (D,), jnp.float32),
        "wq": 2 * weights(kq, D, HEADS * HEAD),
        "wk": 2 * weights(kk, D, KV_HEADS * HEAD),
        "wv": 4 * weights(kv, D, KV_HEADS * HEAD),
        "wo": weights(ko, HEADS * HEAD, D),
    }
    return {k: v.astype(jnp.bfloat16) for k, v in drawn.items()}


def normed(x, gain):
    wide = x.astype(jnp.float32)
    scale = lax.rsqrt(jnp.mean(wide * wide, -1, keepdims=True) + 1e-6)
    return (wide * scale * gain.astype(jnp.float32)).astype(jnp.bfloat16)


def turned(t, place, theta):
    half = t.shape[-1] // 2
    angle = place.astype(jnp.float32)[:, None] * theta ** (-jnp.arange(half, dtype=jnp.float32) / half)
    cos, sin = jnp.cos(angle)[:, None], jnp.sin(angle)[:, None]
    a, b = t[..., :half].astype(jnp.float32), t[..., half:].astype(jnp.float32)
    return jnp.concatenate([a * cos - b * sin, b * cos + a * sin], -1).astype(jnp.bfloat16)


def matmul(a, w):
    return jnp.dot(a, w, preferred_element_type=jnp.float32).astype(jnp.bfloat16)


def einsum(form, a, b):
    return jnp.einsum(form, a.astype(jnp.float32), b.astype(jnp.float32))


def attention(q, k, v):
    scores = einsum("tgsd,ugd->gstu", q, k) * q.shape[-1] ** -0.5
    token = jnp.arange(q.shape[0])
    scores = jnp.where(token[:, None] >= token, scores, -jnp.inf)
    weights = jax.nn.softmax(scores, -1).astype(jnp.bfloat16)
    return einsum("gstu,ugd->tgsd", weights, v).astype(jnp.bfloat16)


def reference(x, gain, wq, wk, wv, wo):
    a, place = normed(x, gain), jnp.arange(ROWS)
    q = turned(matmul(a, wq).reshape(ROWS, HEADS, HEAD), place, THETA).reshape(ROWS, KV_HEADS, -1, HEAD)
    k = turned(matmul(a, wk).reshape(ROWS, KV_HEADS, HEAD), place, THETA)
    v = matmul(a, wv).reshape(ROWS, KV_HEADS, HEAD)
    seen = attention(q, k, v).reshape(ROWS, HEADS * HEAD)
    return (x.astype(jnp.float32) + jnp.dot(seen, wo, preferred_element_type=jnp.float32)).astype(jnp.bfloat16)
```

```python
import jax
import jax.numpy as jnp
import numpy as np
from jax import lax
from jax.experimental import pallas as pl
from jax.experimental.pallas import tpu as pltpu
from jax.sharding import PartitionSpec as P

HEAD = 128
THETA = 10000
NEG = -1e30
HIDDEN = 2 * NEG
LOG2E = 1.4426950408889634
MESH = pl.DeviceIdType.MESH
DEVICES = 8

T = 512
D = 3072
ROWS = D // DEVICES
HALF = D // 2
KH = 4
KW = KH * HEAD
G = 3
SG = 2
SGW = HALF // SG
WC = 6
WCW = D // WC
VIA_X = (4, 5)


def _dot(a, b, ca, cb):
    return lax.dot_general(a, b, (((ca,), (cb,)), ((), ())), preferred_element_type=jnp.float32)


def _kernel(
    x_ref, gain_ref, freq_ref, wq_ref, wk_ref, wv_ref, wo_ref,
    y_ref, wof_ref,
    a_s, xo_s, xr_s, wq_s, wk_s, wv_s, k_s, v_s, q_s, att_s, give_s, cos_s, sin_s, top_s, mix_s, out_s,
    send_sem, recv_sem, local_sem, tile_sem, out_sem,
):
    me = lax.axis_index("sp")
    mx, my, mk = me // 4, (me // 2) % 2, me % 2

    def dev(r):
        x = 1 - mx if r & 4 else mx
        y = 1 - my if r & 2 else my
        k = 1 - mk if r & 1 else mk
        return 4 * x + 2 * y + k

    def wrows(r):
        return pl.ds(pl.multiple_of(dev(r) * ROWS, ROWS), ROWS)

    def half(h, width):
        return pl.ds(pl.multiple_of(h * width, width), width)

    def chunk(c):
        return pl.ds(c * WCW, WCW)

    def place(kind, r, i):
        if kind == "wk":
            return wk_s.at[wrows(r)]
        if kind == "wv":
            return wv_s.at[wrows(r)]
        if kind == "wq":
            return wq_s.at[wrows(r), pl.ds(i * SGW, SGW)]
        if kind == "k":
            return k_s.at[dev(r)]
        if kind == "v":
            return v_s.at[dev(r)]
        if kind == "wo":
            return wof_ref.at[wrows(r), chunk(i)]
        if kind == "x":
            return xr_s
        if kind == "att":
            return give_s.at[:, pl.ds(i * SGW, SGW)]

    def own(kind, h, i):
        if kind == "wk":
            return wk_ref.at[:, half(h, KW)]
        if kind == "wv":
            return wv_ref.at[:, half(h, KW)]
        if kind == "wq":
            return wq_ref.at[:, pl.ds(pl.multiple_of(h * HALF + i * SGW, SGW), SGW)]
        if kind == "wo":
            return wo_ref.at[:, chunk(i)]
        if kind == "x":
            return x_ref
        return place(kind, 0, i)

    recv_index = {}
    for kind, count in (("wk", 1), ("wv", 1), ("wq", SG), ("k", 1), ("v", 1), ("wo", WC)):
        for i in range(count):
            for r in range(1, 8):
                recv_index[kind, r, i] = len(recv_index)
    recv_index["x", 4, 0] = len(recv_index)
    for i in range(SG):
        recv_index["att", 4, i] = len(recv_index)

    started = []

    def send(kind, r, link, i=0):
        src = own(kind, 1 - mx if link == 4 else mx, i) if r == 0 else place(kind, r, i)
        if kind == "att":
            dst = att_s.at[:, pl.ds(pl.multiple_of(mx * HALF + i * SGW, SGW), SGW)]
        else:
            dst = place(kind, r, i)
        copy = pltpu.make_async_remote_copy(
            src_ref=src, dst_ref=dst, send_sem=send_sem.at[len(started)], recv_sem=recv_sem.at[recv_index[kind, r ^ link, i]],
            device_id={"sp": dev(link)}, device_id_type=MESH,
        )
        copy.start()
        started.append(copy)

    def wait(kind, r, i=0):
        if kind == "att":
            dst = att_s.at[:, pl.ds(pl.multiple_of((1 - mx) * HALF + i * SGW, SGW), SGW)]
        else:
            dst = place(kind, r, i)
        pltpu.make_async_remote_copy(
            src_ref=dst, dst_ref=dst, send_sem=send_sem.at[0], recv_sem=recv_sem.at[recv_index[kind, r, i]],
            device_id={"sp": dev(4)}, device_id_type=MESH,
        ).wait_recv()

    barrier = pltpu.get_barrier_semaphore()
    for link in (1, 2, 4):
        pl.semaphore_signal(barrier, 1, device_id={"sp": dev(link)}, device_id_type=MESH)
    pl.semaphore_wait(barrier, 3)

    for kind in ("wk", "wv"):
        send(kind, 0, 4)
        send(kind, 0, 2)
    send("x", 0, 4)
    send("wq", 0, 2, 0)
    for i in range(SG):
        send("wq", 0, 4, i)
    for c in range(WC - 1):
        send("wo", 0, 4, c)
    local = [
        pltpu.make_async_copy(x_ref, xo_s, local_sem.at[0]),
        pltpu.make_async_copy(own("wk", mx, 0), place("wk", 0, 0), local_sem.at[1]),
        pltpu.make_async_copy(own("wv", mx, 0), place("wv", 0, 0), local_sem.at[2]),
        pltpu.make_async_copy(own("wq", mx, 0), place("wq", 0, 0), local_sem.at[3]),
        pltpu.make_async_copy(own("wq", mx, 1), place("wq", 0, 1), local_sem.at[4]),
    ]
    for copy in local:
        copy.start()
    for kind in ("wk", "wv"):
        send(kind, 0, 1)
    for i in range(SG):
        send("wq", 0, 1, i)

    def tables(t, block):
        def body(i, _):
            at = pl.ds(pl.multiple_of(i * 64, 64), 64)
            token = block * T + i * 64 + lax.broadcasted_iota(jnp.int32, (64, HEAD), 0)
            angle = token.astype(jnp.float32) * freq_ref[...]
            cos_s[t, at, :] = jnp.cos(angle)
            sin = jnp.sin(angle)
            lane = lax.broadcasted_iota(jnp.int32, (64, HEAD), 1)
            sin_s[t, at, :] = jnp.where(lane < HEAD // 2, -sin, sin)

        lax.fori_loop(0, T // 64, body, None)

    def norm(src, t):
        def body(i, _):
            at = pl.ds(pl.multiple_of(i * 32, 32), 32)
            wide = src[at, :].astype(jnp.float32)
            scale = lax.rsqrt(jnp.mean(wide * wide, -1, keepdims=True) + 1e-6)
            a_s[t, at, :] = (wide * scale * gain_ref[...].astype(jnp.float32)).astype(jnp.bfloat16)

        lax.fori_loop(0, T // 32, body, None)

    def turned(t, value):
        wide = value.astype(jnp.bfloat16).astype(jnp.float32)
        return (wide * cos_s[t] + pltpu.roll(wide, HEAD // 2, 1) * sin_s[t]).astype(jnp.bfloat16)

    def keys_values(t, block):
        def body(n, _):
            cols = pl.ds(pl.multiple_of(n * 256, 256), 256)
            k = _dot(a_s[t], wk_s[:, cols], 1, 0)
            v = _dot(a_s[t], wv_s[:, cols], 1, 0).astype(jnp.bfloat16)
            for h in range(2):
                lanes = slice(h * HEAD, (h + 1) * HEAD)
                k_s[block, 2 * n + h] = turned(t, k[:, lanes])
                v_s[block, 2 * n + h] = v[:, lanes].T

        lax.fori_loop(0, KW // 256, body, None)

    def queries(t, i):
        def body(n, _):
            cols = pl.ds(pl.multiple_of(i * SGW + n * 256, 256), 256)
            q = _dot(a_s[t], wq_s[:, cols], 1, 0)
            for h in range(2):
                q_s[t, i * (SGW // HEAD) + 2 * n + h] = turned(t, q[:, h * HEAD : (h + 1) * HEAD])

        lax.fori_loop(0, SGW // 256, body, None)

    local[0].wait()
    tables(0, me)
    norm(xo_s, 0)
    tables(1, dev(4))

    def pass_on(kind, r, i=0, links=(1,)):
        wait(kind, r, i)
        for link in links:
            send(kind, r, link, i)

    both = ("wk", "wv")
    for kind in both:
        pass_on(kind, 4, 0, (2, 1))
    send("wq", 0, 2, 1)
    for kind in both:
        pass_on(kind, 2)
    for r in (1, 5, 3):
        for kind in both:
            wait(kind, r)
    for kind in both:
        pass_on(kind, 6)
    for kind in both:
        wait(kind, 7)
    for copy in local[1:3]:
        copy.wait()

    keys_values(0, me)
    for kind in ("k", "v"):
        send(kind, 0, 2)
        send(kind, 0, 1)
    for c in VIA_X:
        send("wo", 0, 2, c)
    for i in range(SG):
        pass_on("wq", 2, i)

    wait("x", 4)
    norm(xr_s, 1)
    keys_values(1, dev(4))
    for kind in ("k", "v"):
        send(kind, 4, 2)
        send(kind, 4, 1)
    for kind in ("k", "v"):
        pass_on(kind, 2)

    for i in range(SG):
        pass_on("wq", 4, i, (2, 1))
    for c in range(WC):
        if c not in VIA_X:
            send("wo", 0, 2, c)
    for c in range(WC):
        send("wo", 0, 1, c)
    local[3].wait()
    local[4].wait()
    for kind in ("k", "v"):
        pass_on(kind, 6)
    for kind in ("k", "v"):
        for r in (1, 5, 3, 7):
            wait(kind, r)

    scale = HEAD**-0.5
    e = scale * LOG2E
    ones = jnp.ones((8, T), jnp.bfloat16)

    def attend(t, i, block, out, base):
        pieces = [(kv, n) for kv in range(KH // SG) for n in range(G)]
        for p in range(len(pieces)):
            top_s[p : p + 1, :] = jnp.full((1, T), NEG, jnp.float32)
            mix_s[p] = jnp.zeros((HEAD + 8, T), jnp.float32)

        def step(j, masked):
            scores = [_dot(k_s[j, i * (KH // SG) + kv], q_s[t, (i * (KH // SG) + kv) * G + n], 1, 1) for kv, n in pieces]
            if masked:
                ok = lax.broadcasted_iota(jnp.int32, (T, T), 0) <= lax.broadcasted_iota(jnp.int32, (T, T), 1)
            weights, keeps = [], []
            for p, s in enumerate(scores):
                if masked:
                    s = jnp.where(ok, s, HIDDEN)
                old = top_s[p : p + 1, :]
                top = jnp.maximum(old, s.max(axis=0, keepdims=True))
                top_s[p : p + 1, :] = top
                weights.append(jnp.exp2((s - top) * e).astype(jnp.bfloat16))
                keeps.append(jnp.exp2((old - top) * e))
            for p, (kv, n) in enumerate(pieces):
                values = jnp.concatenate([v_s[j, i * (KH // SG) + kv], ones], axis=0)
                mix_s[p] = mix_s[p] * keeps[p] + _dot(values, weights[p], 1, 0)

        lax.fori_loop(0, block, lambda j, _: step(j, False), None)
        step(block, True)
        for p in range(len(pieces)):
            total = mix_s[p, HEAD : HEAD + 1, :]
            at = pl.multiple_of(base + p * HEAD, HEAD)
            out[:, pl.ds(at, HEAD)] = (mix_s[p, :HEAD, :] * (1 / total)).T.astype(jnp.bfloat16)

    for i in range(SG):
        for r in (1, 5, 3):
            wait("wq", r, i)
        pass_on("wq", 6, i)
        wait("wq", 7, i)
        for t in range(2):
            queries(t, i)
        attend(1, i, dev(4), give_s, i * SGW)
        send("att", 0, 4, i)
        if i == 0:
            for c in (0, 1):
                pass_on("wo", 4, c, (2, 1))
        else:
            send("wo", 0, 4, WC - 1)
        attend(0, i, me, att_s, mx * HALF + i * SGW)
        if i == 0:
            for c in (2, 3):
                pass_on("wo", 4, c, (2, 1))
            for c in VIA_X:
                pass_on("wo", 2, c, (4, 1))

    for c in range(WC):
        if c in VIA_X:
            pass_on("wo", 4, c)
        else:
            pass_on("wo", 2, c)
    for i in range(SG):
        wait("att", 4, i)
    for copy in started:
        copy.wait_send()
    sent = len(started)
    order = VIA_X + tuple(c for c in range(WC) if c not in VIA_X)

    def loads(n):
        cols = pl.ds(n % 3 * WCW, WCW)
        src = [wo_ref.at[:, chunk(order[n])]] + [place("wo", r, order[n]) for r in range(1, 8)]
        return [
            pltpu.make_async_copy(src[r], wq_s.at[wrows(r), cols], tile_sem.at[n % 3, r])
            for r in range(8)
        ]

    def fetch(n):
        c = order[n]
        pass_on("wo", 6, c)
        for r in (1, 5, 3, 7):
            wait("wo", r, c)
        for copy in loads(n):
            copy.start()

    def write(n):
        return pltpu.make_async_copy(out_s.at[n % 2], y_ref.at[:, chunk(order[n])], out_sem.at[n % 2])

    fetch(0)
    for n, c in enumerate(order):
        if n + 1 < WC - 1:
            fetch(n + 1)
        if n == WC - 1:
            fetch(n)
        for copy in loads(n):
            copy.wait()
        if n >= 2:
            write(n - 2).wait()

        def body(m, _):
            cols = pl.ds(pl.multiple_of(m * 256, 256), 256)
            y = _dot(att_s[...], wq_s[:, pl.ds(pl.multiple_of(n % 3 * WCW + m * 256, 256), 256)], 1, 0)
            x = xo_s[:, pl.ds(pl.multiple_of(c * WCW + m * 256, 256), 256)].astype(jnp.float32)
            out_s[n % 2, :, cols] = (x + y).astype(jnp.bfloat16)

        lax.fori_loop(0, WCW // 256, body, None)
        write(n).start()
    for n in (WC - 2, WC - 1):
        write(n).wait()
    for copy in started[sent:]:
        copy.wait_send()


SENDS = 88
RECVS = 7 * (4 + SG + WC) + 1 + SG


def solution(mesh):
    freq = (THETA ** (-np.arange(HEAD // 2, dtype=np.float32) / (HEAD // 2))).astype(np.float32)
    freq = np.concatenate([freq, freq])[None]
    low = jnp.bfloat16
    vmem = pl.BlockSpec(memory_space=pltpu.VMEM)
    hbm = pl.BlockSpec(memory_space=pl.ANY)

    def step(x, gain, wq, wk, wv, wo):
        y, _ = pl.pallas_call(
            _kernel,
            name="half_layer",
            in_specs=[hbm, vmem, vmem, hbm, hbm, hbm, hbm],
            out_specs=[hbm, hbm],
            out_shape=[jax.ShapeDtypeStruct((T, D), low), jax.ShapeDtypeStruct((D, D), low)],
            scratch_shapes=[
                pltpu.VMEM((2, T, D), low),
                pltpu.VMEM((T, D), low),
                pltpu.VMEM((T, D), low),
                pltpu.VMEM((D, HALF), low),
                pltpu.VMEM((D, KW), low),
                pltpu.VMEM((D, KW), low),
                pltpu.VMEM((DEVICES, KH, T, HEAD), low),
                pltpu.VMEM((DEVICES, KH, HEAD, T), low),
                pltpu.VMEM((2, KH * G, T, HEAD), low),
                pltpu.VMEM((T, D), low),
                pltpu.VMEM((T, HALF), low),
                pltpu.VMEM((2, T, HEAD), jnp.float32),
                pltpu.VMEM((2, T, HEAD), jnp.float32),
                pltpu.VMEM((8, T), jnp.float32),
                pltpu.VMEM((KH // SG * G, HEAD + 8, T), jnp.float32),
                pltpu.VMEM((2, T, WCW), low),
                pltpu.SemaphoreType.DMA((SENDS,)),
                pltpu.SemaphoreType.DMA((RECVS,)),
                pltpu.SemaphoreType.DMA((5,)),
                pltpu.SemaphoreType.DMA((3, 8)),
                pltpu.SemaphoreType.DMA((2,)),
            ],
            compiler_params=pltpu.CompilerParams(collective_id=0, has_side_effects=True, vmem_limit_bytes=67_000_000),
        )(x, gain[None], jnp.asarray(freq), wq, wk, wv, wo)
        return y

    tokens, whole = P(("dp", "sp"), None), P("sp", None)
    return jax.shard_map(
        step,
        mesh=mesh,
        in_specs=(tokens, P(None), whole, whole, whole, whole),
        out_specs=tokens,
        check_vma=False,
    )
```

```python
import jax
import jax.numpy as jnp
import numpy as np
from jax import lax
from jax.experimental import pallas as pl
from jax.experimental.pallas import tpu as pltpu
from jax.sharding import PartitionSpec as P

HEAD = 128
THETA = 10000
NEG = -1e30
HIDDEN = 2 * NEG
LOG2E = 1.4426950408889634
MESH = pl.DeviceIdType.MESH
DEVICES = 8

T = 512
D = 3072
ROWS = D // DEVICES
HALF = D // 2
KH = 4
KW = KH * HEAD
G = 3
SG = 2
SGW = HALF // SG
WC = 6
WCW = D // WC
VIA_X = (4, 5)


def _dot(a, b, ca, cb):
    return lax.dot_general(a, b, (((ca,), (cb,)), ((), ())), preferred_element_type=jnp.float32)


def _kernel(
    x_ref, gain_ref, freq_ref, wq_ref, wk_ref, wv_ref, wo_ref,
    y_ref, wof_ref,
    a_s, xo_s, xr_s, wq_s, wk_s, wv_s, k_s, v_s, q_s, att_s, give_s, cos_s, sin_s, top_s, mix_s, out_s,
    send_sem, recv_sem, local_sem, tile_sem, out_sem,
):
    me = lax.axis_index("sp")
    mx, my, mk = me // 4, (me // 2) % 2, me % 2

    def dev(r):
        x = 1 - mx if r & 4 else mx
        y = 1 - my if r & 2 else my
        k = 1 - mk if r & 1 else mk
        return 4 * x + 2 * y + k

    def wrows(r):
        return pl.ds(pl.multiple_of(dev(r) * ROWS, ROWS), ROWS)

    def half(h, width):
        return pl.ds(pl.multiple_of(h * width, width), width)

    def chunk(c):
        return pl.ds(c * WCW, WCW)

    def place(kind, r, i):
        if kind == "wk":
            return wk_s.at[wrows(r)]
        if kind == "wv":
            return wv_s.at[wrows(r)]
        if kind == "wq":
            return wq_s.at[wrows(r), pl.ds(i * SGW, SGW)]
        if kind == "k":
            return k_s.at[dev(r)]
        if kind == "v":
            return v_s.at[dev(r)]
        if kind == "wo":
            return wof_ref.at[wrows(r), chunk(i)]
        if kind == "x":
            return xr_s
        if kind == "att":
            return give_s.at[:, pl.ds(i * SGW, SGW)]

    def own(kind, h, i):
        if kind == "wk":
            return wk_ref.at[:, half(h, KW)]
        if kind == "wv":
            return wv_ref.at[:, half(h, KW)]
        if kind == "wq":
            return wq_ref.at[:, pl.ds(pl.multiple_of(h * HALF + i * SGW, SGW), SGW)]
        if kind == "wo":
            return wo_ref.at[:, chunk(i)]
        if kind == "x":
            return x_ref
        return place(kind, 0, i)

    recv_index = {}
    for kind, count in (("wk", 1), ("wv", 1), ("wq", SG), ("k", 1), ("v", 1), ("wo", WC)):
        for i in range(count):
            for r in range(1, 8):
                recv_index[kind, r, i] = len(recv_index)
    recv_index["x", 4, 0] = len(recv_index)
    for i in range(SG):
        recv_index["att", 4, i] = len(recv_index)

    started = []

    def send(kind, r, link, i=0):
        src = own(kind, 1 - mx if link == 4 else mx, i) if r == 0 else place(kind, r, i)
        if kind == "att":
            dst = att_s.at[:, pl.ds(pl.multiple_of(mx * HALF + i * SGW, SGW), SGW)]
        else:
            dst = place(kind, r, i)
        copy = pltpu.make_async_remote_copy(
            src_ref=src, dst_ref=dst, send_sem=send_sem.at[len(started)], recv_sem=recv_sem.at[recv_index[kind, r ^ link, i]],
            device_id={"sp": dev(link)}, device_id_type=MESH,
        )
        copy.start()
        started.append((kind, copy))

    def wait(kind, r, i=0):
        if kind == "att":
            dst = att_s.at[:, pl.ds(pl.multiple_of((1 - mx) * HALF + i * SGW, SGW), SGW)]
        else:
            dst = place(kind, r, i)
        pltpu.make_async_remote_copy(
            src_ref=dst, dst_ref=dst, send_sem=send_sem.at[0], recv_sem=recv_sem.at[recv_index[kind, r, i]],
            device_id={"sp": dev(4)}, device_id_type=MESH,
        ).wait_recv()

    barrier = pltpu.get_barrier_semaphore()
    for link in (1, 2, 4):
        pl.semaphore_signal(barrier, 1, device_id={"sp": dev(link)}, device_id_type=MESH)
    pl.semaphore_wait(barrier, 3)

    for kind in ("wk", "wv"):
        send(kind, 0, 4)
        send(kind, 0, 2)
    send("wq", 0, 4, 0)
    send("wq", 0, 2, 0)
    send("x", 0, 4)
    send("wq", 0, 4, 1)
    for c in range(WC):
        send("wo", 0, 4, c)
    local = [
        pltpu.make_async_copy(x_ref, xo_s, local_sem.at[0]),
        pltpu.make_async_copy(own("wk", mx, 0), place("wk", 0, 0), local_sem.at[1]),
        pltpu.make_async_copy(own("wv", mx, 0), place("wv", 0, 0), local_sem.at[2]),
        pltpu.make_async_copy(own("wq", mx, 0), place("wq", 0, 0), local_sem.at[3]),
        pltpu.make_async_copy(own("wq", mx, 1), place("wq", 0, 1), local_sem.at[4]),
    ]
    for copy in local:
        copy.start()
    for kind in ("wk", "wv"):
        send(kind, 0, 1)
    for i in range(SG):
        send("wq", 0, 1, i)

    def tables(t, block):
        def body(i, _):
            at = pl.ds(pl.multiple_of(i * 64, 64), 64)
            token = block * T + i * 64 + lax.broadcasted_iota(jnp.int32, (64, HEAD), 0)
            angle = token.astype(jnp.float32) * freq_ref[...]
            cos_s[t, at, :] = jnp.cos(angle)
            sin = jnp.sin(angle)
            lane = lax.broadcasted_iota(jnp.int32, (64, HEAD), 1)
            sin_s[t, at, :] = jnp.where(lane < HEAD // 2, -sin, sin)

        lax.fori_loop(0, T // 64, body, None)

    def norm(src, t):
        def body(i, _):
            at = pl.ds(pl.multiple_of(i * 32, 32), 32)
            wide = src[at, :].astype(jnp.float32)
            scale = lax.rsqrt(jnp.mean(wide * wide, -1, keepdims=True) + 1e-6)
            a_s[t, at, :] = (wide * scale * gain_ref[...].astype(jnp.float32)[None]).astype(jnp.bfloat16)

        lax.fori_loop(0, T // 32, body, None)

    def turned(t, value):
        wide = value.astype(jnp.bfloat16).astype(jnp.float32)
        return (wide * cos_s[t] + pltpu.roll(wide, HEAD // 2, 1) * sin_s[t]).astype(jnp.bfloat16)

    def keys_values(t, block):
        def body(n, _):
            cols = pl.ds(pl.multiple_of(n * 256, 256), 256)
            k = _dot(a_s[t], wk_s[:, cols], 1, 0)
            v = _dot(a_s[t], wv_s[:, cols], 1, 0).astype(jnp.bfloat16)
            for h in range(2):
                lanes = slice(h * HEAD, (h + 1) * HEAD)
                k_s[block, 2 * n + h] = turned(t, k[:, lanes])
                v_s[block, 2 * n + h] = v[:, lanes].T

        lax.fori_loop(0, KW // 256, body, None)

    def queries(t, i):
        def body(n, _):
            cols = pl.ds(pl.multiple_of(i * SGW + n * 256, 256), 256)
            q = _dot(a_s[t], wq_s[:, cols], 1, 0)
            for h in range(2):
                q_s[t, i * (SGW // HEAD) + 2 * n + h] = turned(t, q[:, h * HEAD : (h + 1) * HEAD])

        lax.fori_loop(0, SGW // 256, body, None)

    local[0].wait()
    tables(0, me)
    norm(xo_s, 0)
    tables(1, dev(4))

    def pass_on(kind, r, i=0, links=(1,)):
        wait(kind, r, i)
        for link in links:
            send(kind, r, link, i)

    both = ("wk", "wv")
    for kind in both:
        pass_on(kind, 4, 0, (2, 1))
    pass_on("wq", 4, 0, (2, 1))
    send("wq", 0, 2, 1)
    for kind in both:
        pass_on(kind, 2)
    for r in (1, 5, 3):
        for kind in both:
            wait(kind, r)
    for kind in both:
        pass_on(kind, 6)
    for kind in both:
        wait(kind, 7)
    for copy in local[1:3]:
        copy.wait()

    keys_values(0, me)
    for kind in ("k", "v"):
        send(kind, 0, 2)
        send(kind, 0, 1)
    for c in VIA_X:
        send("wo", 0, 2, c)
    for c in range(WC):
        send("wo", 0, 1, c)

    def whole_wq(i):
        for r in (1, 5, 3):
            wait("wq", r, i)
        pass_on("wq", 6, i)
        wait("wq", 7, i)
        local[3 + i].wait()

    pass_on("wq", 2, 0)
    whole_wq(0)
    queries(0, 0)
    pass_on("wq", 2, 1)
    for kind in ("k", "v"):
        pass_on(kind, 2)
    wait("x", 4)
    norm(xr_s, 1)
    keys_values(1, dev(4))
    for kind in ("k", "v"):
        send(kind, 4, 2)
        send(kind, 4, 1)
    queries(1, 0)
    pass_on("wq", 4, 1, (2, 1))
    for c in range(WC):
        if c not in VIA_X:
            send("wo", 0, 2, c)
    for kind in ("k", "v"):
        for r in (1, 3, 5):
            wait(kind, r)

    e = HEAD**-0.5 * LOG2E
    ones = jnp.ones((8, T), jnp.bfloat16)
    per = KH // SG
    pieces = [(kv, n) for kv in range(per) for n in range(G)]
    mine = (me, dev(4))

    def begin():
        for t in range(2):
            top_s[t] = jnp.full(top_s.shape[1:], NEG, jnp.float32)
            mix_s[t] = jnp.zeros(mix_s.shape[1:], jnp.float32)

    def step(t, i, j, masked):
        scores = [_dot(k_s[j, i * per + kv], q_s[t, (i * per + kv) * G + n], 1, 1) for kv, n in pieces]
        if masked:
            ok = lax.broadcasted_iota(jnp.int32, (T, T), 0) <= lax.broadcasted_iota(jnp.int32, (T, T), 1)
        weights, keeps = [], []
        for p, s in enumerate(scores):
            if masked:
                s = jnp.where(ok, s, HIDDEN)
            old = top_s[t, p : p + 1, :]
            top = jnp.maximum(old, s.max(axis=0, keepdims=True))
            top_s[t, p : p + 1, :] = top
            weights.append(jnp.exp2((s - top) * e).astype(jnp.bfloat16))
            keeps.append(jnp.exp2((old - top) * e))
        for p, (kv, n) in enumerate(pieces):
            values = jnp.concatenate([v_s[j, i * per + kv], ones], axis=0)
            mix_s[t, p] = mix_s[t, p] * keeps[p] + _dot(values, weights[p], 1, 0)

    def last(t):
        return me + t * (dev(4) - me)

    def some(r):
        x, y, k = r // 4, (r // 2) % 2, r % 2
        return 4 * (mx + x - 2 * mx * x) + 2 * (my + y - 2 * my * y) + mk + k - 2 * mk * k

    def over(count, item, i):
        def body(n, _):
            t, r = item(n)

            @pl.when(some(r) < last(t))
            def _():
                step(t, i, some(r), False)

        lax.fori_loop(0, count, body, None)

    def finish(t, out, base):
        for p in range(len(pieces)):
            total = mix_s[t, p, HEAD : HEAD + 1, :]
            at = pl.multiple_of(base + p * HEAD, HEAD)
            out[:, pl.ds(at, HEAD)] = (mix_s[t, p, :HEAD, :] * (1 / total)).T.astype(jnp.bfloat16)

    def early():
        begin()
        lax.fori_loop(0, 2, lambda t, _: step(t, 0, last(t), True), None)
        over(12, lambda n: (1 - n // 6, n % 6), 0)

    def late():
        over(4, lambda n: (1 - n // 2, 6 + n % 2), 0)
        finish(1, give_s, 0)

    def rest(t):
        step(t, 1, mine[t], True)
        over(8, lambda n: (t, n), 1)

    early()
    for kind in ("k", "v"):
        pass_on(kind, 6)
    for kind in ("k", "v"):
        wait(kind, 7)
    late()
    send("att", 0, 4, 0)
    finish(0, att_s, mx * HALF)
    for c in range(WC):
        if c not in VIA_X:
            pass_on("wo", 4, c, (2, 1))
    whole_wq(1)
    queries(1, 1)
    begin()
    rest(1)
    finish(1, give_s, SGW)
    send("att", 0, 4, 1)
    for c in VIA_X:
        pass_on("wo", 2, c, (4, 1))
    queries(0, 1)
    rest(0)
    finish(0, att_s, mx * HALF + SGW)

    order = (0, 1, 4, 2, 5, 3)
    for c in order:
        if c in VIA_X:
            pass_on("wo", 4, c)
        else:
            pass_on("wo", 2, c)
    for i in range(SG):
        wait("att", 4, i)
    for kind, copy in started:
        if kind in ("wq", "wk", "wv"):
            copy.wait_send()

    def tile(n):
        return (wq_s, 0) if n == WC - 1 else (wq_s, n * WCW) if n < 3 else ((wk_s, 0), (wv_s, 0))[n - 3]

    def load(n, r):
        ref, at = tile(n)
        src = wo_ref.at[:, chunk(order[n])] if r == 0 else place("wo", r, order[n])
        return pltpu.make_async_copy(src, ref.at[wrows(r), pl.ds(at, WCW)], tile_sem.at[n, r])

    def fetch(n):
        for r in (1, 5, 3):
            wait("wo", r, order[n])
        for r in range(6):
            load(n, r).start()

    def write(n):
        return pltpu.make_async_copy(out_s.at[n % 2], y_ref.at[:, chunk(order[n])], out_sem.at[n % 2])

    def project(n, c):
        ref, at = tile(n)

        def body(m, _):
            cols = pl.ds(pl.multiple_of(m * 256, 256), 256)
            y = _dot(att_s[...], ref[:, pl.ds(pl.multiple_of(at + m * 256, 256), 256)], 1, 0)
            x = xo_s[:, pl.ds(pl.multiple_of(c * WCW + m * 256, 256), 256)].astype(jnp.float32)
            out_s[n % 2, :, cols] = (x + y).astype(jnp.bfloat16)

        lax.fori_loop(0, WCW // 256, body, None)

    for n in range(WC - 1):
        fetch(n)
    for n, c in enumerate(order):
        pass_on("wo", 6, c)
        load(n, 6).start()
        wait("wo", 7, c)
        load(n, 7).start()
        for r in range(8):
            load(n, r).wait()
        if n >= 2:
            write(n - 2).wait()
        project(n, c)
        write(n).start()
        if n == 0:
            fetch(WC - 1)
    for n in (WC - 2, WC - 1):
        write(n).wait()
    for kind, copy in started:
        if kind not in ("wq", "wk", "wv"):
            copy.wait_send()


SENDS = 88
RECVS = 7 * (4 + SG + WC) + 1 + SG


def solution(mesh):
    freq = (THETA ** (-np.arange(HEAD // 2, dtype=np.float32) / (HEAD // 2))).astype(np.float32)
    freq = np.concatenate([freq, freq])[None]
    low = jnp.bfloat16
    vmem = pl.BlockSpec(memory_space=pltpu.VMEM)
    hbm = pl.BlockSpec(memory_space=pl.ANY)

    def step(x, gain, wq, wk, wv, wo):
        y, _ = pl.pallas_call(
            _kernel,
            name="half_layer",
            in_specs=[hbm, vmem, vmem, hbm, hbm, hbm, hbm],
            out_specs=[hbm, hbm],
            out_shape=[jax.ShapeDtypeStruct((T, D), low), jax.ShapeDtypeStruct((D, D), low)],
            scratch_shapes=[
                pltpu.VMEM((2, T, D), low),
                pltpu.VMEM((T, D), low),
                pltpu.VMEM((T, D), low),
                pltpu.VMEM((D, HALF), low),
                pltpu.VMEM((D, KW), low),
                pltpu.VMEM((D, KW), low),
                pltpu.VMEM((DEVICES, KH, T, HEAD), low),
                pltpu.VMEM((DEVICES, KH, HEAD, T), low),
                pltpu.VMEM((2, KH * G, T, HEAD), low),
                pltpu.VMEM((T, D), low),
                pltpu.VMEM((T, HALF), low),
                pltpu.VMEM((2, T, HEAD), jnp.float32),
                pltpu.VMEM((2, T, HEAD), jnp.float32),
                pltpu.VMEM((2, 8, T), jnp.float32),
                pltpu.VMEM((2, KH // SG * G, HEAD + 8, T), jnp.float32),
                pltpu.VMEM((2, T, WCW), low),
                pltpu.SemaphoreType.DMA((SENDS,)),
                pltpu.SemaphoreType.DMA((RECVS,)),
                pltpu.SemaphoreType.DMA((5,)),
                pltpu.SemaphoreType.DMA((WC, 8)),
                pltpu.SemaphoreType.DMA((2,)),
            ],
            compiler_params=pltpu.CompilerParams(collective_id=0, has_side_effects=True, vmem_limit_bytes=67_000_000),
        )(x, gain, jnp.asarray(freq), wq, wk, wv, wo)
        return y

    tokens, whole = P(("dp", "sp"), None), P("sp", None)
    return jax.shard_map(
        step,
        mesh=mesh,
        in_specs=(tokens, P(None), whole, whole, whole, whole),
        out_specs=tokens,
        check_vma=False,
    )
```

```python
import jax
import jax.numpy as jnp
import numpy as np
from jax import lax
from jax.experimental import pallas as pl
from jax.experimental.pallas import tpu as pltpu
from jax.sharding import PartitionSpec as P

HEAD = 128
THETA = 10000
NEG = -1e30
HIDDEN = 2 * NEG
LOG2E = 1.4426950408889634
MESH = pl.DeviceIdType.MESH
DEVICES = 8

T = 512
D = 3072
ROWS = D // DEVICES
HALF = D // 2
KH = 4
KW = KH * HEAD
G = 3
SG = 2
SGW = HALF // SG
WO = ((0, 512, "y"), (512, 512, "y"), (1024, 512, "y"), (1536, 256, "y"), (1792, 256, "y"), (2048, 512, "x"), (2560, 256, "x"), (2816, 256, "x"))
FINAL = 4
TILES = {0: ("wq", 0), 1: ("wq", 512), 5: ("wq", 1024), 2: ("wk", 0), 6: ("wv", 0), 3: ("wv", 256), 7: ("wq", 0)}
EARLY_X = ()
FIRST_X = (0, 1, 2, 3, 4, 5)
FIRST_Y = (5, 6, 7)
STEPS = (("pass", 0), ("load", 0), ("done", 0), ("pass", 1), ("load", 1), ("done", 1), ("pass", 5), ("load", 5), ("pass", 2), ("done", 5), ("load", 2), ("pass", 6), ("done", 2), ("load", 6), ("pass", 3), ("pass", 7), ("load", 3), ("done", 6), ("load", 7), ("done", 3), ("pass", 4), ("done", 7))
ORDER = (0, 1, 5, 2, 6, 3, 7)


def _dot(a, b, ca, cb):
    return lax.dot_general(a, b, (((ca,), (cb,)), ((), ())), preferred_element_type=jnp.float32)


def _kernel(
    x_ref, gain_ref, freq_ref, wq_ref, wk_ref, wv_ref, wo_ref,
    y_ref, att_ref, wof_ref,
    a_s, xo_s, xr_s, wq_s, wk_s, wv_s, k_s, v_s, q_s, att_s, give_s, cos_s, sin_s, top_s, mix_s, out_s, sum_s, part_s, came_s,
    send_sem, recv_sem, local_sem, tile_sem, out_sem,
):
    me = lax.axis_index("sp")
    mx, my, mk = me // 4, (me // 2) % 2, me % 2

    def dev(r):
        x = 1 - mx if r & 4 else mx
        y = 1 - my if r & 2 else my
        k = 1 - mk if r & 1 else mk
        return 4 * x + 2 * y + k

    def wrows(r):
        return pl.ds(pl.multiple_of(dev(r) * ROWS, ROWS), ROWS)

    def half(h, width):
        return pl.ds(pl.multiple_of(h * width, width), width)

    def chunk(c):
        return pl.ds(WO[c][0], WO[c][1])

    def ways(*which):
        return tuple(c for c in range(len(WO)) if WO[c][2] in which)

    def place(kind, r, i):
        if kind == "wk":
            return wk_s.at[wrows(r)]
        if kind == "wv":
            return wv_s.at[wrows(r)]
        if kind == "wq":
            return wq_s.at[wrows(r), pl.ds(i * SGW, SGW)]
        if kind == "k":
            return k_s.at[dev(r)]
        if kind == "v":
            return v_s.at[dev(r)]
        if kind == "wo":
            return wof_ref.at[wrows(r), chunk(i)]
        if kind == "x":
            return xr_s
        if kind == "att":
            return give_s.at[:, pl.ds(i * SGW, SGW)]
        if kind == "sum":
            return part_s.at[ways("r").index(i)]

    def own(kind, h, i):
        if kind == "wk":
            return wk_ref.at[:, half(h, KW)]
        if kind == "wv":
            return wv_ref.at[:, half(h, KW)]
        if kind == "wq":
            return wq_ref.at[:, pl.ds(pl.multiple_of(h * HALF + i * SGW, SGW), SGW)]
        if kind == "wo":
            return wo_ref.at[:, chunk(i)]
        if kind == "x":
            return x_ref
        return place(kind, 0, i)

    recv_index = {}
    for kind, count in (("wk", 1), ("wv", 1), ("wq", SG), ("k", 1), ("v", 1), ("wo", len(WO))):
        for i in range(count):
            for r in range(1, 4 if kind == "wo" and WO[i][2] == "r" else 8):
                recv_index[kind, r, i] = len(recv_index)
    for c in ways("r"):
        recv_index["sum", 4, c] = len(recv_index)
    recv_index["x", 4, 0] = len(recv_index)
    for i in range(SG):
        recv_index["att", 4, i] = len(recv_index)

    started = []

    def send(kind, r, link, i=0):
        src = own(kind, 1 - mx if link == 4 else mx, i) if r == 0 else place(kind, r, i)
        if kind == "att":
            dst = att_s.at[:, pl.ds(pl.multiple_of(mx * HALF + i * SGW, SGW), SGW)]
        else:
            dst = place(kind, r, i)
        copy = pltpu.make_async_remote_copy(
            src_ref=src, dst_ref=dst, send_sem=send_sem.at[len(started)], recv_sem=recv_sem.at[recv_index[kind, r ^ link, i]],
            device_id={"sp": dev(link)}, device_id_type=MESH,
        )
        copy.start()
        started.append((kind, copy))

    def wait(kind, r, i=0):
        if kind == "att":
            dst = att_s.at[:, pl.ds(pl.multiple_of((1 - mx) * HALF + i * SGW, SGW), SGW)]
        else:
            dst = place(kind, r, i)
        pltpu.make_async_remote_copy(
            src_ref=dst, dst_ref=dst, send_sem=send_sem.at[0], recv_sem=recv_sem.at[recv_index[kind, r, i]],
            device_id={"sp": dev(4)}, device_id_type=MESH,
        ).wait_recv()

    barrier = pltpu.get_barrier_semaphore()
    for link in (1, 2, 4):
        pl.semaphore_signal(barrier, 1, device_id={"sp": dev(link)}, device_id_type=MESH)
    pl.semaphore_wait(barrier, 3)

    for kind in ("wk", "wv"):
        send(kind, 0, 4)
        send(kind, 0, 2)
    send("wq", 0, 4, 0)
    send("wq", 0, 2, 0)
    send("x", 0, 4)
    send("wq", 0, 4, 1)
    for c in FIRST_X:
        send("wo", 0, 4, c)
    local = [
        pltpu.make_async_copy(x_ref, xo_s, local_sem.at[0]),
        pltpu.make_async_copy(own("wk", mx, 0), place("wk", 0, 0), local_sem.at[1]),
        pltpu.make_async_copy(own("wv", mx, 0), place("wv", 0, 0), local_sem.at[2]),
        pltpu.make_async_copy(own("wq", mx, 0), place("wq", 0, 0), local_sem.at[3]),
        pltpu.make_async_copy(own("wq", mx, 1), place("wq", 0, 1), local_sem.at[4]),
    ]
    for copy in local:
        copy.start()
    for kind in ("wk", "wv"):
        send(kind, 0, 1)
    for i in range(SG):
        send("wq", 0, 1, i)

    def tables(t, block):
        def body(i, _):
            at = pl.ds(pl.multiple_of(i * 64, 64), 64)
            token = block * T + i * 64 + lax.broadcasted_iota(jnp.int32, (64, HEAD), 0)
            angle = token.astype(jnp.float32) * freq_ref[...]
            cos_s[t, at, :] = jnp.cos(angle)
            sin = jnp.sin(angle)
            lane = lax.broadcasted_iota(jnp.int32, (64, HEAD), 1)
            sin_s[t, at, :] = jnp.where(lane < HEAD // 2, -sin, sin)

        lax.fori_loop(0, T // 64, body, None)

    def norm(src, t):
        def body(i, _):
            at = pl.ds(pl.multiple_of(i * 32, 32), 32)
            wide = src[at, :].astype(jnp.float32)
            scale = lax.rsqrt(jnp.mean(wide * wide, -1, keepdims=True) + 1e-6)
            a_s[t, at, :] = (wide * scale * gain_ref[...].astype(jnp.float32)[None]).astype(jnp.bfloat16)

        lax.fori_loop(0, T // 32, body, None)

    def turned(t, value):
        wide = value.astype(jnp.bfloat16).astype(jnp.float32)
        return (wide * cos_s[t] + pltpu.roll(wide, HEAD // 2, 1) * sin_s[t]).astype(jnp.bfloat16)

    def keys_values(t, block):
        def body(n, _):
            cols = pl.ds(pl.multiple_of(n * 256, 256), 256)
            k = _dot(a_s[t], wk_s[:, cols], 1, 0)
            v = _dot(a_s[t], wv_s[:, cols], 1, 0).astype(jnp.bfloat16)
            for h in range(2):
                lanes = slice(h * HEAD, (h + 1) * HEAD)
                k_s[block, 2 * n + h] = turned(t, k[:, lanes])
                v_s[block, 2 * n + h] = v[:, lanes].T

        lax.fori_loop(0, KW // 256, body, None)

    def queries(t, i):
        def body(n, _):
            cols = pl.ds(pl.multiple_of(i * SGW + n * 256, 256), 256)
            q = _dot(a_s[t], wq_s[:, cols], 1, 0)
            for h in range(2):
                q_s[t, i * (SGW // HEAD) + 2 * n + h] = turned(t, q[:, h * HEAD : (h + 1) * HEAD])

        lax.fori_loop(0, SGW // 256, body, None)

    local[0].wait()
    tables(0, me)
    norm(xo_s, 0)
    tables(1, dev(4))

    def pass_on(kind, r, i=0, links=(1,)):
        wait(kind, r, i)
        for link in links:
            send(kind, r, link, i)

    both = ("wk", "wv")
    for kind in both:
        pass_on(kind, 4, 0, (2, 1))
    pass_on("wq", 4, 0, (2, 1))
    send("wq", 0, 2, 1)
    for kind in both:
        pass_on(kind, 2)
    for r in (1, 5, 3):
        for kind in both:
            wait(kind, r)
    for kind in both:
        pass_on(kind, 6)
    for kind in both:
        wait(kind, 7)
    for copy in local[1:3]:
        copy.wait()

    keys_values(0, me)
    for kind in ("k", "v"):
        send(kind, 0, 2)
        send(kind, 0, 1)
    for c in FIRST_Y:
        send("wo", 0, 2, c)
    for c in range(len(WO)):
        send("wo", 0, 1, c)

    def whole_wq(i):
        for r in (1, 5, 3):
            wait("wq", r, i)
        pass_on("wq", 6, i)
        wait("wq", 7, i)
        local[3 + i].wait()

    pass_on("wq", 2, 0)
    whole_wq(0)
    queries(0, 0)
    pass_on("wq", 2, 1)
    for kind in ("k", "v"):
        pass_on(kind, 2)
    wait("x", 4)
    norm(xr_s, 1)
    keys_values(1, dev(4))
    for kind in ("k", "v"):
        send(kind, 4, 2)
        send(kind, 4, 1)
    queries(1, 0)
    pass_on("wq", 4, 1, (2, 1))
    for c in ways("r", "y"):
        if c not in FIRST_Y:
            send("wo", 0, 2, c)
    for c in EARLY_X:
        pass_on("wo", 2, c, (4, 1))
    for kind in ("k", "v"):
        for r in (1, 3, 5):
            wait(kind, r)

    e = HEAD**-0.5 * LOG2E
    ones = jnp.ones((8, T), jnp.bfloat16)
    per = KH // SG
    pieces = [(kv, n) for kv in range(per) for n in range(G)]
    mine = (me, dev(4))

    def begin():
        for t in range(2):
            top_s[t] = jnp.full(top_s.shape[1:], NEG, jnp.float32)
            mix_s[t] = jnp.zeros(mix_s.shape[1:], jnp.float32)

    def step(t, i, j, masked):
        scores = [_dot(k_s[j, i * per + kv], q_s[t, (i * per + kv) * G + n], 1, 1) for kv, n in pieces]
        if masked:
            ok = lax.broadcasted_iota(jnp.int32, (T, T), 0) <= lax.broadcasted_iota(jnp.int32, (T, T), 1)
        weights, keeps = [], []
        for p, s in enumerate(scores):
            if masked:
                s = jnp.where(ok, s, HIDDEN)
            old = top_s[t, p : p + 1, :]
            top = jnp.maximum(old, s.max(axis=0, keepdims=True))
            top_s[t, p : p + 1, :] = top
            weights.append(jnp.exp2((s - top) * e).astype(jnp.bfloat16))
            keeps.append(jnp.exp2((old - top) * e))
        for p, (kv, n) in enumerate(pieces):
            values = jnp.concatenate([v_s[j, i * per + kv], ones], axis=0)
            mix_s[t, p] = mix_s[t, p] * keeps[p] + _dot(values, weights[p], 1, 0)

    def last(t):
        return me + t * (dev(4) - me)

    def some(r):
        x, y, k = r // 4, (r // 2) % 2, r % 2
        return 4 * (mx + x - 2 * mx * x) + 2 * (my + y - 2 * my * y) + mk + k - 2 * mk * k

    def over(count, item, i):
        def body(n, _):
            t, r = item(n)

            @pl.when(some(r) < last(t))
            def _():
                step(t, i, some(r), False)

        lax.fori_loop(0, count, body, None)

    def finish(t, out, base):
        for p in range(len(pieces)):
            total = mix_s[t, p, HEAD : HEAD + 1, :]
            at = pl.multiple_of(base + p * HEAD, HEAD)
            out[:, pl.ds(at, HEAD)] = (mix_s[t, p, :HEAD, :] * (1 / total)).T.astype(jnp.bfloat16)

    def early():
        begin()
        lax.fori_loop(0, 2, lambda t, _: step(t, 0, last(t), True), None)
        over(12, lambda n: (1 - n // 6, n % 6), 0)

    def late():
        over(4, lambda n: (1 - n // 2, 6 + n % 2), 0)
        finish(1, give_s, 0)

    def rest(t):
        step(t, 1, mine[t], True)
        over(8, lambda n: (t, n), 1)

    early()
    for kind in ("k", "v"):
        pass_on(kind, 6)
    for kind in ("k", "v"):
        wait(kind, 7)
    late()
    send("att", 0, 4, 0)
    finish(0, att_s, mx * HALF)
    for c in ways("y"):
        pass_on("wo", 4, c, (2, 1))
    whole_wq(1)
    queries(1, 1)
    begin()
    rest(1)
    finish(1, give_s, SGW)
    send("att", 0, 4, 1)
    for c in ways("y", "x"):
        if c not in FIRST_X:
            send("wo", 0, 4, c)
    for c in ways("x"):
        if c not in EARLY_X:
            pass_on("wo", 2, c, (4, 1))

    for kind, copy in started:
        if kind in ("wk", "wv"):
            copy.wait_send()
    half_rows = lambda n, r: pl.ds(pl.multiple_of(n * HALF + (dev(r) - 4 * mx) * ROWS, ROWS), ROWS)

    def half_load(n, r):
        c = ways("r")[n]
        src = wo_ref.at[:, chunk(c)] if r == 0 else place("wo", r, c)
        return pltpu.make_async_copy(src, wk_s.at[half_rows(n, r), :], tile_sem.at[c, r])

    def half_sum(rows, n, m):
        w = wk_s[pl.ds(n * HALF, HALF), pl.ds(pl.multiple_of(m * 256, 256), 256)]
        return _dot(rows, w, 1, 0)

    for n, c in enumerate(ways("r")):
        pass_on("wo", 2, c)
        for r in (1, 3):
            wait("wo", r, c)
        for r in range(4):
            half_load(n, r).start()
    for n, c in enumerate(ways("r")):
        for r in range(4):
            half_load(n, r).wait()

        def body(m, _):
            part_s[n, :, pl.ds(pl.multiple_of(m * 256, 256), 256)] = half_sum(give_s[...], n, m).astype(jnp.bfloat16)

        lax.fori_loop(0, WO[c][1] // 256, body, None)
        send("sum", 0, 4, c)

    queries(0, 1)
    rest(0)
    finish(0, att_s, mx * HALF + SGW)

    for n, c in enumerate(ways("r")):

        def body(m, _):
            mine = att_s[:, pl.ds(pl.multiple_of(mx * HALF, HALF), HALF)]
            sum_s[n, :, pl.ds(pl.multiple_of(m * 256, 256), 256)] = half_sum(mine, n, m)

        lax.fori_loop(0, WO[c][1] // 256, body, None)

    for c in ways("x"):
        if c in FIRST_X:
            pass_on("wo", 4, c)
    for c in ways("y"):
        pass_on("wo", 2, c)
    for kind, copy in started:
        if kind == "wq":
            copy.wait_send()

    def tile(c):
        kind, at = TILES[c]
        return {"wq": wq_s, "wk": wk_s, "wv": wv_s}[kind], at

    def load(c, r):
        ref, at = tile(c)
        src = wo_ref.at[:, chunk(c)] if r == 0 else place("wo", r, c)
        return pltpu.make_async_copy(src, ref.at[wrows(r), pl.ds(at, WO[c][1])], tile_sem.at[c, r])

    def late_rows(c):
        return (6,) if WO[c][2] == "y" or c in FIRST_X else (4, 6)

    def fetch(c):
        for r in (1, 5, 3):
            if r ^ 1 not in late_rows(c):
                wait("wo", r, c)
        for r in range(6):
            if r & 6 not in late_rows(c):
                load(c, r).start()

    def write(n):
        c = ORDER[n]
        return pltpu.make_async_copy(out_s.at[n % 2, :, pl.ds(0, WO[c][1])], y_ref.at[:, chunk(c)], out_sem.at[n % 2])

    def project(n, c):
        def body(m, _):
            cols = pl.ds(pl.multiple_of(m * 256, 256), 256)
            if WO[c][2] == "r":
                i = ways("r").index(c)
                y = sum_s[i, :, cols] + came_s[i, :, cols].astype(jnp.float32)
            else:
                ref, at = tile(c)
                y = _dot(att_s[...], ref[:, pl.ds(pl.multiple_of(at + m * 256, 256), 256)], 1, 0)
            x = xo_s[:, pl.ds(pl.multiple_of(WO[c][0] + m * 256, 256), 256)].astype(jnp.float32)
            out_s[n % 2, :, cols] = (x + y).astype(jnp.bfloat16)

        lax.fori_loop(0, WO[c][1] // 256, body, None)

    def complete(c):
        for r in late_rows(c):
            pass_on("wo", r, c)
            if c in TILES:
                load(c, r).start()

    whole = tuple(c for c in ORDER if WO[c][2] != "r")
    after = {c: d for d in whole for c in whole if whole.index(c) < whole.index(d) and TILES[c] == TILES[d]}
    for c in whole:
        if c not in after.values():
            fetch(c)
    for i in range(SG):
        wait("att", 4, i)
    kept = pltpu.make_async_copy(att_s, att_ref, local_sem.at[0])
    kept.start()
    for what, c in STEPS:
        n = ORDER.index(c) if c in ORDER else None
        if what == "pass":
            complete(c)
        elif what == "load":
            for r in late_rows(c):
                wait("wo", r + 1, c)
                load(c, r + 1).start()
        else:
            if WO[c][2] == "r":
                wait("sum", 4, c)
            else:
                for r in range(8):
                    load(c, r).wait()
            if n >= 2:
                write(n - 2).wait()
            project(n, c)
            write(n).start()
            if c in after:
                fetch(after[c])
    for r in (1, 5, 3, 7):
        wait("wo", r, FINAL)
    for n in (len(ORDER) - 2, len(ORDER) - 1):
        write(n).wait()
    kept.wait()
    for kind, copy in started:
        if kind not in ("wq", "wk", "wv"):
            copy.wait_send()


def _last(x_ref, wo_ref, part_ref, att_ref, wof_ref, y_ref, y_s, x_s, att_s, w_s, in_sem, out_sem):
    me = lax.axis_index("sp")
    start, width, _ = WO[FINAL]
    cols = pl.ds(start, width)
    others = [pl.ds(WO[c][0], WO[c][1]) for c in ORDER]
    copies = [pltpu.make_async_copy(att_ref, att_s, in_sem.at[0]), pltpu.make_async_copy(x_ref.at[:, cols], x_s, in_sem.at[1])]
    for r in range(DEVICES):
        d = lax.rem(me + r, DEVICES)
        at = pl.ds(pl.multiple_of(d * ROWS, ROWS), ROWS)
        copies.append(pltpu.make_async_copy(wo_ref.at[:, cols] if r == 0 else wof_ref.at[at, cols], w_s.at[at], in_sem.at[2 + r]))
    for copy in copies:
        copy.start()
    moved = [pltpu.make_async_copy(part_ref.at[:, o], y_s.at[:, o], in_sem.at[10 + n]) for n, o in enumerate(others)]
    for copy in moved:
        copy.start()
    for copy in copies:
        copy.wait()
    y_s[:, cols] = (x_s[...].astype(jnp.float32) + _dot(att_s[...], w_s[...], 1, 0)).astype(jnp.bfloat16)
    outs = [pltpu.make_async_copy(y_s.at[:, o], y_ref.at[:, o], out_sem.at[n]) for n, o in enumerate(others + [cols])]
    for n, copy in enumerate(moved):
        copy.wait()
        outs[n].start()
    outs[-1].start()
    for copy in outs:
        copy.wait()


RS = sum(way == "r" for _, _, way in WO)
SENDS = 7 * (4 + SG + len(WO)) - 4 * RS + 1 + SG + RS - 2
RECVS = 7 * (4 + SG + len(WO)) - 4 * RS + 1 + SG + RS


def solution(mesh):
    freq = (THETA ** (-np.arange(HEAD // 2, dtype=np.float32) / (HEAD // 2))).astype(np.float32)
    freq = np.concatenate([freq, freq])[None]
    low = jnp.bfloat16
    vmem = pl.BlockSpec(memory_space=pltpu.VMEM)
    hbm = pl.BlockSpec(memory_space=pl.ANY)

    def step(x, gain, wq, wk, wv, wo):
        part, att, gathered = pl.pallas_call(
            _kernel,
            name="half_layer",
            in_specs=[hbm, vmem, vmem, hbm, hbm, hbm, hbm],
            out_specs=[hbm, hbm, hbm],
            out_shape=[jax.ShapeDtypeStruct((T, D), low), jax.ShapeDtypeStruct((T, D), low), jax.ShapeDtypeStruct((D, D), low)],
            scratch_shapes=[
                pltpu.VMEM((2, T, D), low),
                pltpu.VMEM((T, D), low),
                pltpu.VMEM((T, D), low),
                pltpu.VMEM((D, HALF), low),
                pltpu.VMEM((D, KW), low),
                pltpu.VMEM((D, KW), low),
                pltpu.VMEM((DEVICES, KH, T, HEAD), low),
                pltpu.VMEM((DEVICES, KH, HEAD, T), low),
                pltpu.VMEM((2, KH * G, T, HEAD), low),
                pltpu.VMEM((T, D), low),
                pltpu.VMEM((T, HALF), low),
                pltpu.VMEM((2, T, HEAD), jnp.float32),
                pltpu.VMEM((2, T, HEAD), jnp.float32),
                pltpu.VMEM((2, 8, T), jnp.float32),
                pltpu.VMEM((2, KH // SG * G, HEAD + 8, T), jnp.float32),
                pltpu.VMEM((2, T, 512), low),
                pltpu.VMEM((max(RS, 1), T, 512), jnp.float32),
                pltpu.VMEM((max(RS, 1), T, 512), low),
                pltpu.VMEM((max(RS, 1), T, 512), low),
                pltpu.SemaphoreType.DMA((SENDS,)),
                pltpu.SemaphoreType.DMA((RECVS,)),
                pltpu.SemaphoreType.DMA((5,)),
                pltpu.SemaphoreType.DMA((len(WO), 8)),
                pltpu.SemaphoreType.DMA((2,)),
            ],
            compiler_params=pltpu.CompilerParams(collective_id=0, has_side_effects=True, vmem_limit_bytes=67_000_000),
        )(x, gain, jnp.asarray(freq), wq, wk, wv, wo)
        return pl.pallas_call(
            _last,
            name="last_columns",
            in_specs=[hbm] * 5,
            out_specs=hbm,
            out_shape=jax.ShapeDtypeStruct((T, D), low),
            scratch_shapes=[
                pltpu.VMEM((T, D), low),
                pltpu.VMEM((T, WO[FINAL][1]), low),
                pltpu.VMEM((T, D), low),
                pltpu.VMEM((D, WO[FINAL][1]), low),
                pltpu.SemaphoreType.DMA((10 + len(ORDER),)),
                pltpu.SemaphoreType.DMA((len(WO),)),
            ],
            compiler_params=pltpu.CompilerParams(vmem_limit_bytes=67_000_000),
        )(x, wo, part, att, gathered)

    tokens, whole = P(("dp", "sp"), None), P("sp", None)
    return jax.shard_map(
        step,
        mesh=mesh,
        in_specs=(tokens, P(None), whole, whole, whole, whole),
        out_specs=tokens,
        check_vma=False,
    )
```

```python
import jax
import jax.numpy as jnp
import numpy as np
from jax import lax
from jax.experimental import pallas as pl
from jax.experimental.pallas import tpu as pltpu
from jax.sharding import PartitionSpec as P

HEAD = 128
THETA = 10000
NEG = -1e30
HIDDEN = 2 * NEG
LOG2E = 1.4426950408889634
MESH = pl.DeviceIdType.MESH
DEVICES = 8

T = 512
D = 3072
ROWS = D // DEVICES
HALF = D // 2
KH = 4
KW = KH * HEAD
G = 3
SG = 2
SGW = HALF // SG
WO = ((0, 512, "y"), (512, 512, "y"), (1024, 256, "y"), (1280, 256, "y"), (1536, 256, "x"), (1792, 256, "x"), (2048, 512, "r"), (2560, 512, "r"))
FINAL = 3
TILES = {0: ("wq", 0), 1: ("wq", 512), 4: ("wq", 1024), 5: ("wq", 1280), 2: ("wv", 0)}
EARLY_X = (4, 5)
FIRST_X = (0, 1, 2, 3, 4, 5)
FIRST_Y = (4, 5, 6)
STEPS = (("pass", 4), ("pass", 5), ("load", 4), ("load", 5), ("done", 4), ("done", 5), ("pass", 0), ("load", 0), ("done", 0), ("pass", 1), ("load", 1), ("done", 6), ("done", 1), ("pass", 2), ("load", 2), ("done", 2), ("pass", 3), ("done", 7))
ORDER = (4, 5, 0, 6, 1, 2, 7)


def _dot(a, b, ca, cb):
    return lax.dot_general(a, b, (((ca,), (cb,)), ((), ())), preferred_element_type=jnp.float32)


def _kernel(
    x_ref, gain_ref, freq_ref, wq_ref, wk_ref, wv_ref, wo_ref,
    y_ref, att_ref, wof_ref,
    a_s, xo_s, xr_s, wq_s, wk_s, wv_s, k_s, v_s, q_s, att_s, give_s, cos_s, sin_s, top_s, mix_s, out_s, sum_s, part_s, came_s,
    send_sem, recv_sem, local_sem, tile_sem, out_sem,
):
    me = lax.axis_index("sp")
    mx, my, mk = me // 4, (me // 2) % 2, me % 2

    def dev(r):
        x = 1 - mx if r & 4 else mx
        y = 1 - my if r & 2 else my
        k = 1 - mk if r & 1 else mk
        return 4 * x + 2 * y + k

    def wrows(r):
        return pl.ds(pl.multiple_of(dev(r) * ROWS, ROWS), ROWS)

    def half(h, width):
        return pl.ds(pl.multiple_of(h * width, width), width)

    def chunk(c):
        return pl.ds(WO[c][0], WO[c][1])

    def ways(*which):
        return tuple(c for c in range(len(WO)) if WO[c][2] in which)

    def place(kind, r, i):
        if kind == "wk":
            return wk_s.at[wrows(r)]
        if kind == "wv":
            return wv_s.at[wrows(r)]
        if kind == "wq":
            return wq_s.at[wrows(r), pl.ds(i * SGW, SGW)]
        if kind == "k":
            return k_s.at[dev(r)]
        if kind == "v":
            return v_s.at[dev(r)]
        if kind == "wo":
            return wof_ref.at[wrows(r), chunk(i)]
        if kind == "x":
            return xr_s
        if kind == "att":
            return give_s.at[:, pl.ds(i * SGW, SGW)]
        if kind == "sum":
            return part_s.at[ways("r").index(i)]

    def own(kind, h, i):
        if kind == "wk":
            return wk_ref.at[:, half(h, KW)]
        if kind == "wv":
            return wv_ref.at[:, half(h, KW)]
        if kind == "wq":
            return wq_ref.at[:, pl.ds(pl.multiple_of(h * HALF + i * SGW, SGW), SGW)]
        if kind == "wo":
            return wo_ref.at[:, chunk(i)]
        if kind == "x":
            return x_ref
        return place(kind, 0, i)

    recv_index = {}
    for kind, count in (("wk", 1), ("wv", 1), ("wq", SG), ("k", 1), ("v", 1), ("wo", len(WO))):
        for i in range(count):
            for r in range(1, 4 if kind == "wo" and WO[i][2] == "r" else 8):
                recv_index[kind, r, i] = len(recv_index)
    for c in ways("r"):
        recv_index["sum", 4, c] = len(recv_index)
    recv_index["x", 4, 0] = len(recv_index)
    for i in range(SG):
        recv_index["att", 4, i] = len(recv_index)

    started = []

    def send(kind, r, link, i=0):
        src = own(kind, 1 - mx if link == 4 else mx, i) if r == 0 else place(kind, r, i)
        if kind == "att":
            dst = att_s.at[:, pl.ds(pl.multiple_of(mx * HALF + i * SGW, SGW), SGW)]
        elif kind == "sum":
            dst = came_s.at[ways("r").index(i)]
        else:
            dst = place(kind, r, i)
        copy = pltpu.make_async_remote_copy(
            src_ref=src, dst_ref=dst, send_sem=send_sem.at[len(started)], recv_sem=recv_sem.at[recv_index[kind, r ^ link, i]],
            device_id={"sp": dev(link)}, device_id_type=MESH,
        )
        copy.start()
        started.append((kind, copy))

    def wait(kind, r, i=0):
        if kind == "att":
            dst = att_s.at[:, pl.ds(pl.multiple_of((1 - mx) * HALF + i * SGW, SGW), SGW)]
        elif kind == "sum":
            dst = came_s.at[ways("r").index(i)]
        else:
            dst = place(kind, r, i)
        pltpu.make_async_remote_copy(
            src_ref=dst, dst_ref=dst, send_sem=send_sem.at[0], recv_sem=recv_sem.at[recv_index[kind, r, i]],
            device_id={"sp": dev(4)}, device_id_type=MESH,
        ).wait_recv()

    barrier = pltpu.get_barrier_semaphore()
    for link in (1, 2, 4):
        pl.semaphore_signal(barrier, 1, device_id={"sp": dev(link)}, device_id_type=MESH)
    pl.semaphore_wait(barrier, 3)

    for kind in ("wk", "wv"):
        send(kind, 0, 4)
        send(kind, 0, 2)
    send("wq", 0, 4, 0)
    send("wq", 0, 2, 0)
    send("x", 0, 4)
    send("wq", 0, 4, 1)
    for c in FIRST_X:
        send("wo", 0, 4, c)
    local = [
        pltpu.make_async_copy(x_ref, xo_s, local_sem.at[0]),
        pltpu.make_async_copy(own("wk", mx, 0), place("wk", 0, 0), local_sem.at[1]),
        pltpu.make_async_copy(own("wv", mx, 0), place("wv", 0, 0), local_sem.at[2]),
        pltpu.make_async_copy(own("wq", mx, 0), place("wq", 0, 0), local_sem.at[3]),
        pltpu.make_async_copy(own("wq", mx, 1), place("wq", 0, 1), local_sem.at[4]),
    ]
    for copy in local:
        copy.start()
    for kind in ("wk", "wv"):
        send(kind, 0, 1)
    for i in range(SG):
        send("wq", 0, 1, i)

    def tables(t, block):
        def body(i, _):
            at = pl.ds(pl.multiple_of(i * 64, 64), 64)
            token = block * T + i * 64 + lax.broadcasted_iota(jnp.int32, (64, HEAD), 0)
            angle = token.astype(jnp.float32) * freq_ref[...]
            cos_s[t, at, :] = jnp.cos(angle)
            sin = jnp.sin(angle)
            lane = lax.broadcasted_iota(jnp.int32, (64, HEAD), 1)
            sin_s[t, at, :] = jnp.where(lane < HEAD // 2, -sin, sin)

        lax.fori_loop(0, T // 64, body, None)

    def norm(src, t):
        def body(i, _):
            at = pl.ds(pl.multiple_of(i * 32, 32), 32)
            wide = src[at, :].astype(jnp.float32)
            scale = lax.rsqrt(jnp.mean(wide * wide, -1, keepdims=True) + 1e-6)
            a_s[t, at, :] = (wide * scale * gain_ref[...].astype(jnp.float32)[None]).astype(jnp.bfloat16)

        lax.fori_loop(0, T // 32, body, None)

    def turned(t, value):
        wide = value.astype(jnp.bfloat16).astype(jnp.float32)
        return (wide * cos_s[t] + pltpu.roll(wide, HEAD // 2, 1) * sin_s[t]).astype(jnp.bfloat16)

    def keys_values(t, block):
        def body(n, _):
            cols = pl.ds(pl.multiple_of(n * 256, 256), 256)
            k = _dot(a_s[t], wk_s[:, cols], 1, 0)
            v = _dot(a_s[t], wv_s[:, cols], 1, 0).astype(jnp.bfloat16)
            for h in range(2):
                lanes = slice(h * HEAD, (h + 1) * HEAD)
                k_s[block, 2 * n + h] = turned(t, k[:, lanes])
                v_s[block, 2 * n + h] = v[:, lanes].T

        lax.fori_loop(0, KW // 256, body, None)

    def queries(t, i):
        def body(n, _):
            cols = pl.ds(pl.multiple_of(i * SGW + n * 256, 256), 256)
            q = _dot(a_s[t], wq_s[:, cols], 1, 0)
            for h in range(2):
                q_s[t, i * (SGW // HEAD) + 2 * n + h] = turned(t, q[:, h * HEAD : (h + 1) * HEAD])

        lax.fori_loop(0, SGW // 256, body, None)

    local[0].wait()
    tables(0, me)
    norm(xo_s, 0)
    tables(1, dev(4))

    def pass_on(kind, r, i=0, links=(1,)):
        wait(kind, r, i)
        for link in links:
            send(kind, r, link, i)

    both = ("wk", "wv")
    for kind in both:
        pass_on(kind, 4, 0, (2, 1))
    pass_on("wq", 4, 0, (2, 1))
    send("wq", 0, 2, 1)
    for kind in both:
        pass_on(kind, 2)
    for r in (1, 5, 3):
        for kind in both:
            wait(kind, r)
    for kind in both:
        pass_on(kind, 6)
    for kind in both:
        wait(kind, 7)
    for copy in local[1:3]:
        copy.wait()

    keys_values(0, me)
    for kind in ("k", "v"):
        send(kind, 0, 2)
        send(kind, 0, 1)
    for c in FIRST_Y:
        send("wo", 0, 2, c)
    for c in range(len(WO)):
        send("wo", 0, 1, c)

    def whole_wq(i):
        for r in (1, 5, 3):
            wait("wq", r, i)
        pass_on("wq", 6, i)
        wait("wq", 7, i)
        local[3 + i].wait()

    pass_on("wq", 2, 0)
    whole_wq(0)
    queries(0, 0)
    pass_on("wq", 2, 1)
    for kind in ("k", "v"):
        pass_on(kind, 2)
    wait("x", 4)
    norm(xr_s, 1)
    keys_values(1, dev(4))
    for kind in ("k", "v"):
        send(kind, 4, 2)
        send(kind, 4, 1)
    queries(1, 0)
    pass_on("wq", 4, 1, (2, 1))
    for c in ways("r") + ways("y"):
        if c not in FIRST_Y:
            send("wo", 0, 2, c)
    for c in EARLY_X:
        pass_on("wo", 2, c, (4, 1))
    for kind in ("k", "v"):
        for r in (1, 3, 5):
            wait(kind, r)

    e = HEAD**-0.5 * LOG2E
    ones = jnp.ones((8, T), jnp.bfloat16)
    per = KH // SG
    pieces = [(kv, n) for kv in range(per) for n in range(G)]
    mine = (me, dev(4))

    def begin():
        for t in range(2):
            top_s[t] = jnp.full(top_s.shape[1:], NEG, jnp.float32)
            mix_s[t] = jnp.zeros(mix_s.shape[1:], jnp.float32)

    def step(t, i, j, masked):
        scores = [_dot(k_s[j, i * per + kv], q_s[t, (i * per + kv) * G + n], 1, 1) for kv, n in pieces]
        if masked:
            ok = lax.broadcasted_iota(jnp.int32, (T, T), 0) <= lax.broadcasted_iota(jnp.int32, (T, T), 1)
        weights, keeps = [], []
        for p, s in enumerate(scores):
            if masked:
                s = jnp.where(ok, s, HIDDEN)
            old = top_s[t, p : p + 1, :]
            top = jnp.maximum(old, s.max(axis=0, keepdims=True))
            top_s[t, p : p + 1, :] = top
            weights.append(jnp.exp2((s - top) * e).astype(jnp.bfloat16))
            keeps.append(jnp.exp2((old - top) * e))
        for p, (kv, n) in enumerate(pieces):
            values = jnp.concatenate([v_s[j, i * per + kv], ones], axis=0)
            mix_s[t, p] = mix_s[t, p] * keeps[p] + _dot(values, weights[p], 1, 0)

    def last(t):
        return me + t * (dev(4) - me)

    def some(r):
        x, y, k = r // 4, (r // 2) % 2, r % 2
        return 4 * (mx + x - 2 * mx * x) + 2 * (my + y - 2 * my * y) + mk + k - 2 * mk * k

    def over(count, item, i):
        def body(n, _):
            t, r = item(n)

            @pl.when(some(r) < last(t))
            def _():
                step(t, i, some(r), False)

        lax.fori_loop(0, count, body, None)

    def finish(t, out, base):
        for p in range(len(pieces)):
            total = mix_s[t, p, HEAD : HEAD + 1, :]
            at = pl.multiple_of(base + p * HEAD, HEAD)
            out[:, pl.ds(at, HEAD)] = (mix_s[t, p, :HEAD, :] * (1 / total)).T.astype(jnp.bfloat16)

    def early():
        begin()
        lax.fori_loop(0, 2, lambda t, _: step(t, 0, last(t), True), None)
        over(12, lambda n: (1 - n // 6, n % 6), 0)

    def late():
        over(4, lambda n: (1 - n // 2, 6 + n % 2), 0)
        finish(1, give_s, 0)

    def rest(t):
        step(t, 1, mine[t], True)
        over(8, lambda n: (t, n), 1)

    early()
    for kind in ("k", "v"):
        pass_on(kind, 6)
    for kind in ("k", "v"):
        wait(kind, 7)
    late()
    send("att", 0, 4, 0)
    finish(0, att_s, mx * HALF)
    for c in ways("y"):
        pass_on("wo", 4, c, (2, 1))
    whole_wq(1)
    queries(1, 1)
    begin()
    rest(1)
    finish(1, give_s, SGW)
    send("att", 0, 4, 1)
    for c in ways("y", "x"):
        if c not in FIRST_X:
            send("wo", 0, 4, c)
    for c in ways("x"):
        if c not in EARLY_X:
            pass_on("wo", 2, c, (4, 1))

    for kind, copy in started:
        if kind in ("wk", "wv"):
            copy.wait_send()
    half_rows = lambda n, r: pl.ds(pl.multiple_of(n * HALF + (dev(r) - 4 * mx) * ROWS, ROWS), ROWS)

    def half_load(n, r):
        c = ways("r")[n]
        src = wo_ref.at[:, chunk(c)] if r == 0 else place("wo", r, c)
        return pltpu.make_async_copy(src, wk_s.at[half_rows(n, r), :], tile_sem.at[c, r])

    def half_sum(rows, n, m):
        w = wk_s[pl.ds(n * HALF, HALF), pl.ds(pl.multiple_of(m * 256, 256), 256)]
        return _dot(rows, w, 1, 0)

    for n, c in enumerate(ways("r")):
        pass_on("wo", 2, c)
        for r in (1, 3):
            wait("wo", r, c)
        for r in range(4):
            half_load(n, r).start()
    for n, c in enumerate(ways("r")):
        for r in range(4):
            half_load(n, r).wait()

        def body(m, _):
            part_s[n, :, pl.ds(pl.multiple_of(m * 256, 256), 256)] = half_sum(give_s[...], n, m).astype(jnp.bfloat16)

        lax.fori_loop(0, WO[c][1] // 256, body, None)
        send("sum", 0, 4, c)

    queries(0, 1)
    rest(0)
    finish(0, att_s, mx * HALF + SGW)

    for n, c in enumerate(ways("r")):

        def body(m, _):
            mine = att_s[:, pl.ds(pl.multiple_of(mx * HALF, HALF), HALF)]
            sum_s[n, :, pl.ds(pl.multiple_of(m * 256, 256), 256)] = half_sum(mine, n, m)

        lax.fori_loop(0, WO[c][1] // 256, body, None)

    for c in ways("x"):
        if c in FIRST_X:
            pass_on("wo", 4, c)
    for c in ways("y"):
        pass_on("wo", 2, c)
    for kind, copy in started:
        if kind == "wq":
            copy.wait_send()

    def tile(c):
        kind, at = TILES[c]
        return {"wq": wq_s, "wk": wk_s, "wv": wv_s}[kind], at

    def load(c, r):
        ref, at = tile(c)
        src = wo_ref.at[:, chunk(c)] if r == 0 else place("wo", r, c)
        return pltpu.make_async_copy(src, ref.at[wrows(r), pl.ds(at, WO[c][1])], tile_sem.at[c, r])

    def late_rows(c):
        return (6,) if WO[c][2] == "y" or c in FIRST_X else (4, 6)

    def fetch(c):
        for r in (1, 5, 3):
            if r ^ 1 not in late_rows(c):
                wait("wo", r, c)
        for r in range(6):
            if r & 6 not in late_rows(c):
                load(c, r).start()

    def write(n):
        c = ORDER[n]
        return pltpu.make_async_copy(out_s.at[n % 2, :, pl.ds(0, WO[c][1])], y_ref.at[:, chunk(c)], out_sem.at[n % 2])

    def project(n, c):
        def body(m, _):
            cols = pl.ds(pl.multiple_of(m * 256, 256), 256)
            if WO[c][2] == "r":
                i = ways("r").index(c)
                y = sum_s[i, :, cols] + came_s[i, :, cols].astype(jnp.float32)
            else:
                ref, at = tile(c)
                y = _dot(att_s[...], ref[:, pl.ds(pl.multiple_of(at + m * 256, 256), 256)], 1, 0)
            x = xo_s[:, pl.ds(pl.multiple_of(WO[c][0] + m * 256, 256), 256)].astype(jnp.float32)
            out_s[n % 2, :, cols] = (x + y).astype(jnp.bfloat16)

        lax.fori_loop(0, WO[c][1] // 256, body, None)

    def complete(c):
        for r in late_rows(c):
            pass_on("wo", r, c)
            if c in TILES:
                load(c, r).start()

    whole = tuple(c for c in ORDER if WO[c][2] != "r")
    after = {c: d for d in whole for c in whole if whole.index(c) < whole.index(d) and TILES[c] == TILES[d]}
    for c in whole:
        if c not in after.values():
            fetch(c)
    for i in range(SG):
        wait("att", 4, i)
    kept = pltpu.make_async_copy(att_s, att_ref, local_sem.at[0])
    kept.start()
    for what, c in STEPS:
        n = ORDER.index(c) if c in ORDER else None
        if what == "pass":
            complete(c)
        elif what == "load":
            for r in late_rows(c):
                wait("wo", r + 1, c)
                load(c, r + 1).start()
        else:
            if WO[c][2] == "r":
                wait("sum", 4, c)
            else:
                for r in range(8):
                    load(c, r).wait()
            if n >= 2:
                write(n - 2).wait()
            project(n, c)
            write(n).start()
            if c in after:
                fetch(after[c])
    for r in (1, 5, 3, 7):
        wait("wo", r, FINAL)
    for n in (len(ORDER) - 2, len(ORDER) - 1):
        write(n).wait()
    kept.wait()
    for kind, copy in started:
        if kind not in ("wq", "wk", "wv"):
            copy.wait_send()


def _last(x_ref, wo_ref, part_ref, att_ref, wof_ref, y_ref, y_s, x_s, att_s, w_s, in_sem, out_sem):
    me = lax.axis_index("sp")
    start, width, _ = WO[FINAL]
    cols = pl.ds(start, width)
    others = [pl.ds(WO[c][0], WO[c][1]) for c in ORDER]
    copies = [pltpu.make_async_copy(att_ref, att_s, in_sem.at[0]), pltpu.make_async_copy(x_ref.at[:, cols], x_s, in_sem.at[1])]
    for r in range(DEVICES):
        d = lax.rem(me + r, DEVICES)
        at = pl.ds(pl.multiple_of(d * ROWS, ROWS), ROWS)
        copies.append(pltpu.make_async_copy(wo_ref.at[:, cols] if r == 0 else wof_ref.at[at, cols], w_s.at[at], in_sem.at[2 + r]))
    for copy in copies:
        copy.start()
    moved = [pltpu.make_async_copy(part_ref.at[:, o], y_s.at[:, o], in_sem.at[10 + n]) for n, o in enumerate(others)]
    for copy in moved:
        copy.start()
    for copy in copies:
        copy.wait()
    y_s[:, cols] = (x_s[...].astype(jnp.float32) + _dot(att_s[...], w_s[...], 1, 0)).astype(jnp.bfloat16)
    outs = [pltpu.make_async_copy(y_s.at[:, o], y_ref.at[:, o], out_sem.at[n]) for n, o in enumerate(others + [cols])]
    for n, copy in enumerate(moved):
        copy.wait()
        outs[n].start()
    outs[-1].start()
    for copy in outs:
        copy.wait()


RS = sum(way == "r" for _, _, way in WO)
SENDS = 7 * (4 + SG + len(WO)) - 4 * RS + 1 + SG + RS - 2
RECVS = 7 * (4 + SG + len(WO)) - 4 * RS + 1 + SG + RS


def solution(mesh):
    freq = (THETA ** (-np.arange(HEAD // 2, dtype=np.float32) / (HEAD // 2))).astype(np.float32)
    freq = np.concatenate([freq, freq])[None]
    low = jnp.bfloat16
    vmem = pl.BlockSpec(memory_space=pltpu.VMEM)
    hbm = pl.BlockSpec(memory_space=pl.ANY)

    def step(x, gain, wq, wk, wv, wo):
        part, att, gathered = pl.pallas_call(
            _kernel,
            name="half_layer",
            in_specs=[hbm, vmem, vmem, hbm, hbm, hbm, hbm],
            out_specs=[hbm, hbm, hbm],
            out_shape=[jax.ShapeDtypeStruct((T, D), low), jax.ShapeDtypeStruct((T, D), low), jax.ShapeDtypeStruct((D, D), low)],
            scratch_shapes=[
                pltpu.VMEM((2, T, D), low),
                pltpu.VMEM((T, D), low),
                pltpu.VMEM((T, D), low),
                pltpu.VMEM((D, HALF), low),
                pltpu.VMEM((D, KW), low),
                pltpu.VMEM((D, KW), low),
                pltpu.VMEM((DEVICES, KH, T, HEAD), low),
                pltpu.VMEM((DEVICES, KH, HEAD, T), low),
                pltpu.VMEM((2, KH * G, T, HEAD), low),
                pltpu.VMEM((T, D), low),
                pltpu.VMEM((T, HALF), low),
                pltpu.VMEM((2, T, HEAD), jnp.float32),
                pltpu.VMEM((2, T, HEAD), jnp.float32),
                pltpu.VMEM((2, 8, T), jnp.float32),
                pltpu.VMEM((2, KH // SG * G, HEAD + 8, T), jnp.float32),
                pltpu.VMEM((2, T, 512), low),
                pltpu.VMEM((max(RS, 1), T, 512), jnp.float32),
                pltpu.VMEM((max(RS, 1), T, 512), low),
                pltpu.VMEM((max(RS, 1), T, 512), low),
                pltpu.SemaphoreType.DMA((SENDS,)),
                pltpu.SemaphoreType.DMA((RECVS,)),
                pltpu.SemaphoreType.DMA((5,)),
                pltpu.SemaphoreType.DMA((len(WO), 8)),
                pltpu.SemaphoreType.DMA((2,)),
            ],
            compiler_params=pltpu.CompilerParams(collective_id=0, has_side_effects=True, vmem_limit_bytes=67_000_000),
        )(x, gain, jnp.asarray(freq), wq, wk, wv, wo)
        return pl.pallas_call(
            _last,
            name="last_columns",
            in_specs=[hbm] * 5,
            out_specs=hbm,
            out_shape=jax.ShapeDtypeStruct((T, D), low),
            scratch_shapes=[
                pltpu.VMEM((T, D), low),
                pltpu.VMEM((T, WO[FINAL][1]), low),
                pltpu.VMEM((T, D), low),
                pltpu.VMEM((D, WO[FINAL][1]), low),
                pltpu.SemaphoreType.DMA((10 + len(ORDER),)),
                pltpu.SemaphoreType.DMA((len(WO),)),
            ],
            compiler_params=pltpu.CompilerParams(vmem_limit_bytes=67_000_000),
        )(x, wo, part, att, gathered)

    tokens, whole = P(("dp", "sp"), None), P("sp", None)
    return jax.shard_map(
        step,
        mesh=mesh,
        in_specs=(tokens, P(None), whole, whole, whole, whole),
        out_specs=tokens,
        check_vma=False,
    )
```

```python
import jax
import jax.numpy as jnp
import numpy as np
from jax import lax
from jax.experimental import pallas as pl
from jax.experimental.pallas import tpu as pltpu
from jax.sharding import PartitionSpec as P

HEAD = 128
THETA = 10000
NEG = -1e30
HIDDEN = 2 * NEG
LOG2E = 1.4426950408889634
MESH = pl.DeviceIdType.MESH
DEVICES = 8

T = 512
D = 3072
ROWS = D // DEVICES
HALF = D // 2
KH = 4
KW = KH * HEAD
G = 3
SG = 2
SGW = HALF // SG
WO = ((0, 512, "y"), (512, 512, "y"), (1024, 256, "y"), (1280, 256, "y"), (1536, 256, "x"), (1792, 256, "x"), (2048, 512, "r"), (2560, 512, "r"))
TILES = {0: ("wq", 0), 1: ("wq", 512), 4: ("wq", 1024), 5: ("wq", 1280), 2: ("wv", 0), 3: ("wv", 256)}
EARLY_X = (4, 5)
FIRST_X = (0, 1, 2, 3, 4, 5)
FIRST_Y = (4, 5)
STEPS = (("pass", 4), ("pass", 5), ("load", 4), ("load", 5), ("done", 4), ("done", 5), ("pass", 0), ("load", 0), ("done", 0), ("pass", 1), ("load", 1), ("done", 6), ("done", 1), ("pass", 2), ("load", 2), ("pass", 3), ("done", 2), ("load", 3), ("done", 7), ("done", 3))
ORDER = (4, 5, 0, 6, 1, 2, 7, 3)


def _dot(a, b, ca, cb):
    return lax.dot_general(a, b, (((ca,), (cb,)), ((), ())), preferred_element_type=jnp.float32)


def _kernel(
    x_ref, gain_ref, freq_ref, wq_ref, wk_ref, wv_ref, wo_ref,
    y_ref, wof_ref,
    a_s, xo_s, xr_s, wq_s, wk_s, wv_s, k_s, v_s, q_s, att_s, give_s, cos_s, sin_s, top_s, mix_s, out_s, sum_s, part_s, came_s,
    send_sem, recv_sem, local_sem, tile_sem, out_sem,
):
    me = lax.axis_index("sp")
    mx, my, mk = me // 4, (me // 2) % 2, me % 2

    def dev(r):
        x = 1 - mx if r & 4 else mx
        y = 1 - my if r & 2 else my
        k = 1 - mk if r & 1 else mk
        return 4 * x + 2 * y + k

    def wrows(r):
        return pl.ds(pl.multiple_of(dev(r) * ROWS, ROWS), ROWS)

    def half(h, width):
        return pl.ds(pl.multiple_of(h * width, width), width)

    def chunk(c):
        return pl.ds(WO[c][0], WO[c][1])

    def ways(*which):
        return tuple(c for c in range(len(WO)) if WO[c][2] in which)

    def place(kind, r, i):
        if kind == "wk":
            return wk_s.at[wrows(r)]
        if kind == "wv":
            return wv_s.at[wrows(r)]
        if kind == "wq":
            return wq_s.at[wrows(r), pl.ds(i * SGW, SGW)]
        if kind == "k":
            return k_s.at[dev(r)]
        if kind == "v":
            return v_s.at[dev(r)]
        if kind == "wo":
            return wof_ref.at[wrows(r), chunk(i)]
        if kind == "x":
            return xr_s
        if kind == "att":
            return give_s.at[:, pl.ds(i * SGW, SGW)]
        if kind == "sum":
            return part_s.at[ways("r").index(i)]

    def own(kind, h, i):
        if kind == "wk":
            return wk_ref.at[:, half(h, KW)]
        if kind == "wv":
            return wv_ref.at[:, half(h, KW)]
        if kind == "wq":
            return wq_ref.at[:, pl.ds(pl.multiple_of(h * HALF + i * SGW, SGW), SGW)]
        if kind == "wo":
            return wo_ref.at[:, chunk(i)]
        if kind == "x":
            return x_ref
        return place(kind, 0, i)

    recv_index = {}

    def recv(kind, r, i):
        key = (kind, r, i)
        if r % 2 and kind in ("wk", "wv"):
            key = ("w", 1, 0)
        elif r % 2 and kind == "wq":
            key = ("wq", 1, i)
        elif r % 2 and kind in ("k", "v"):
            key = ("kv", {1: 1, 3: 3, 5: 3, 7: 7}[r], 0)
        elif r in (1, 3, 5) and kind == "wo":
            key = ("wo", 1, i)
        return recv_sem.at[recv_index.setdefault(key, len(recv_index))]

    def wait_shared(kind, r, i, like):
        sem = recv(kind, r, i)
        pltpu.make_async_remote_copy(
            src_ref=like, dst_ref=like, send_sem=send_sem.at[0], recv_sem=sem, device_id={"sp": dev(4)}, device_id_type=MESH
        ).wait_recv()

    taken = []
    started, settled, free = [], [], list(range(SENDS))

    def settle(which):
        for n, (kind, link, copy) in enumerate(started):
            if n not in settled and which(kind, link):
                copy.wait_send()
                settled.append(n)
                free.append(taken[n])

    def send(kind, r, link, i=0):
        src = own(kind, 1 - mx if link == 4 else mx, i) if r == 0 else place(kind, r, i)
        if kind == "att":
            dst = att_s.at[:, pl.ds(pl.multiple_of(mx * HALF + i * SGW, SGW), SGW)]
        elif kind == "sum":
            dst = came_s.at[ways("r").index(i)]
        else:
            dst = place(kind, r, i)
        taken.append(free.pop(free.index(min(free))))
        copy = pltpu.make_async_remote_copy(
            src_ref=src, dst_ref=dst, send_sem=send_sem.at[taken[-1]], recv_sem=recv(kind, r ^ link, i),
            device_id={"sp": dev(link)}, device_id_type=MESH,
        )
        copy.start()
        started.append((kind, link, copy))

    def wait(kind, r, i=0):
        if kind == "att":
            dst = att_s.at[:, pl.ds(pl.multiple_of((1 - mx) * HALF + i * SGW, SGW), SGW)]
        elif kind == "sum":
            dst = came_s.at[ways("r").index(i)]
        else:
            dst = place(kind, r, i)
        pltpu.make_async_remote_copy(
            src_ref=dst, dst_ref=dst, send_sem=send_sem.at[0], recv_sem=recv(kind, r, i),
            device_id={"sp": dev(4)}, device_id_type=MESH,
        ).wait_recv()

    barrier = pltpu.get_barrier_semaphore()
    for link in (1, 2, 4):
        pl.semaphore_signal(barrier, 1, device_id={"sp": dev(link)}, device_id_type=MESH)
    pl.semaphore_wait(barrier, 3)

    for kind in ("wk", "wv"):
        send(kind, 0, 4)
        send(kind, 0, 2)
    for i in range(SG):
        send("wq", 0, 4, i)
    send("wq", 0, 2, 0)
    send("x", 0, 4)
    for c in FIRST_X:
        send("wo", 0, 4, c)
    local = [
        pltpu.make_async_copy(x_ref, xo_s, local_sem.at[0]),
        pltpu.make_async_copy(own("wk", mx, 0), place("wk", 0, 0), local_sem.at[1]),
        pltpu.make_async_copy(own("wv", mx, 0), place("wv", 0, 0), local_sem.at[2]),
        pltpu.make_async_copy(own("wq", mx, 0), place("wq", 0, 0), local_sem.at[3]),
        pltpu.make_async_copy(own("wq", mx, 1), place("wq", 0, 1), local_sem.at[4]),
    ]
    for copy in local:
        copy.start()
    for kind in ("wk", "wv"):
        send(kind, 0, 1)
    for i in range(SG):
        send("wq", 0, 1, i)

    def tables(t, block):
        def body(i, _):
            at = pl.ds(pl.multiple_of(i * 64, 64), 64)
            token = block * T + i * 64 + lax.broadcasted_iota(jnp.int32, (64, HEAD), 0)
            angle = token.astype(jnp.float32) * freq_ref[...]
            cos_s[t, at, :] = jnp.cos(angle)
            sin = jnp.sin(angle)
            lane = lax.broadcasted_iota(jnp.int32, (64, HEAD), 1)
            sin_s[t, at, :] = jnp.where(lane < HEAD // 2, -sin, sin)

        lax.fori_loop(0, T // 64, body, None)

    def norm(src, t):
        def body(i, _):
            at = pl.ds(pl.multiple_of(i * 32, 32), 32)
            wide = src[at, :].astype(jnp.float32)
            scale = lax.rsqrt(jnp.mean(wide * wide, -1, keepdims=True) + 1e-6)
            a_s[t, at, :] = (wide * scale * gain_ref[...].astype(jnp.float32)[None]).astype(jnp.bfloat16)

        lax.fori_loop(0, T // 32, body, None)

    def turned(t, value):
        wide = value.astype(jnp.bfloat16).astype(jnp.float32)
        return (wide * cos_s[t] + pltpu.roll(wide, HEAD // 2, 1) * sin_s[t]).astype(jnp.bfloat16)

    def keys_values(t, block):
        def body(n, _):
            cols = pl.ds(pl.multiple_of(n * 256, 256), 256)
            k = _dot(a_s[t], wk_s[:, cols], 1, 0)
            v = _dot(a_s[t], wv_s[:, cols], 1, 0).astype(jnp.bfloat16)
            for h in range(2):
                lanes = slice(h * HEAD, (h + 1) * HEAD)
                k_s[block, 2 * n + h] = turned(t, k[:, lanes])
                v_s[block, 2 * n + h] = v[:, lanes].T

        lax.fori_loop(0, KW // 256, body, None)

    def queries(t, i):
        def body(n, _):
            cols = pl.ds(pl.multiple_of(i * SGW + n * 256, 256), 256)
            q = _dot(a_s[t], wq_s[:, cols], 1, 0)
            for h in range(2):
                q_s[t, i * (SGW // HEAD) + 2 * n + h] = turned(t, q[:, h * HEAD : (h + 1) * HEAD])

        lax.fori_loop(0, SGW // 256, body, None)

    local[0].wait()
    tables(0, me)
    norm(xo_s, 0)
    tables(1, dev(4))

    def pass_on(kind, r, i=0, links=(1,)):
        wait(kind, r, i)
        for link in links:
            send(kind, r, link, i)

    both = ("wk", "wv")
    for kind in both:
        pass_on(kind, 4, 0, (2, 1))
    pass_on("wq", 4, 0, (2, 1))
    send("wq", 0, 2, 1)
    pass_on("wq", 4, 1, (2, 1))
    for kind in both:
        pass_on(kind, 2)
    for kind in both:
        pass_on(kind, 6)
    wait_shared("wk", 1, 0, wk_s)
    settle(lambda kind, link: link == 1)
    for copy in local[1:3]:
        copy.wait()

    keys_values(0, me)
    for kind in ("k", "v"):
        send(kind, 0, 2)
        send(kind, 0, 1)
    for c in FIRST_Y:
        send("wo", 0, 2, c)
    for c in range(len(WO)):
        send("wo", 0, 1, c)

    def whole_wq(i):
        pass_on("wq", 6, i)
        wait_shared("wq", 1, i, wq_s.at[pl.ds(0, D // 2), pl.ds(i * SGW, SGW)])
        local[3 + i].wait()

    def whole_wq(i):
        pass_on("wq", 6, i)
        wait_shared("wq", 1, i, wq_s.at[pl.ds(0, D // 2), pl.ds(i * SGW, SGW)])
        local[3 + i].wait()

    e = HEAD**-0.5 * LOG2E
    ones = jnp.ones((8, T), jnp.bfloat16)
    per = KH // SG
    pieces = [(kv, n) for kv in range(per) for n in range(G)]
    mine = (me, dev(4))

    def begin():
        top_s[...] = jnp.full(top_s.shape, NEG, jnp.float32)

        def body(n, _):
            mix_s[n // SG, n % SG] = jnp.zeros(mix_s.shape[2:], jnp.float32)

        lax.fori_loop(0, 2 * SG, body, None)

    def step(t, i, j, masked):
        scores = [_dot(k_s[j, i * per + kv], q_s[t, (i * per + kv) * G + n], 1, 1) for kv, n in pieces]
        if masked:
            ok = lax.broadcasted_iota(jnp.int32, (T, T), 0) <= lax.broadcasted_iota(jnp.int32, (T, T), 1)
        weights, keeps = [], []
        for p, s in enumerate(scores):
            if masked:
                s = jnp.where(ok, s, HIDDEN)
            old = top_s[t, i, p : p + 1, :]
            top = jnp.maximum(old, s.max(axis=0, keepdims=True))
            top_s[t, i, p : p + 1, :] = top
            weights.append(jnp.exp2((s - top) * e).astype(jnp.bfloat16))
            keeps.append(jnp.exp2((old - top) * e))
        for p, (kv, n) in enumerate(pieces):
            values = jnp.concatenate([v_s[j, i * per + kv], ones], axis=0)
            mix_s[t, i, p] = mix_s[t, i, p] * keeps[p] + _dot(values, weights[p], 1, 0)

    def last(t):
        return me + t * (dev(4) - me)

    def some(r):
        x, y, k = r // 4, (r // 2) % 2, r % 2
        return 4 * (mx + x - 2 * mx * x) + 2 * (my + y - 2 * my * y) + mk + k - 2 * mk * k

    def over(first, count, item):
        def body(n, _):
            t, i, r = item(n)

            @pl.when(some(r) < last(t))
            def _():
                step(t, i, some(r), False)

        lax.fori_loop(first, count, body, None)

    def diagonal(t):
        lax.fori_loop(0, SG, lambda i, _: step(t, i, mine[t], True), None)

    def finish(t, i, out, base):
        for p in range(len(pieces)):
            total = mix_s[t, i, p, HEAD : HEAD + 1, :]
            at = pl.multiple_of(base + i * SGW + p * HEAD, HEAD)
            out[:, pl.ds(at, HEAD)] = (mix_s[t, i, p, :HEAD, :] * (1 / total)).T.astype(jnp.bfloat16)

    def near():
        begin()
        diagonal(0)
        over(0, SG, lambda n: (0, n, 1))

    def early(first, count):
        over(first, count, lambda n: (1, n // 5, (5 + n % 5) % 6))

    def late(i):
        over(6, 8, lambda n: (1, i, n))
        finish(1, i, give_s, 0)

    def rest(first, count):
        over(first, count, lambda n: (0, n % SG, 2 + n // SG))

    ahead = 2 * SG * mx

    for i in range(SG):
        pass_on("wq", 2, i)
        whole_wq(i)
        queries(0, i)
    wait_shared("k", 1, 0, k_s.at[pl.ds(0, 2)])
    near()
    settle(lambda kind, link: kind in ("wk", "wv", "wq"))
    wait("x", 4)
    norm(xr_s, 1)
    keys_values(1, dev(4))
    for kind in ("k", "v"):
        send(kind, 4, 2)
        send(kind, 4, 1)
    for c in ways("r") + ways("y"):
        if c not in FIRST_Y:
            send("wo", 0, 2, c)
    for kind in ("k", "v"):
        pass_on(kind, 2)
    for c in EARLY_X:
        pass_on("wo", 2, c, (4, 1))
    for i in range(SG):
        queries(1, i)
    wait_shared("k", 3, 0, k_s.at[pl.ds(0, 4)])
    settle(lambda kind, link: link == 1 or kind == "x")
    diagonal(1)
    early(0, 7)
    rest(0, ahead)
    for kind in ("k", "v"):
        pass_on(kind, 6)
    wait_shared("k", 7, 0, k_s.at[pl.ds(0, 2)])
    late(0)
    send("att", 0, 4, 0)
    early(7, 10)
    late(1)
    send("att", 0, 4, 1)
    for c in ways("y", "x"):
        if c not in FIRST_X:
            send("wo", 0, 4, c)
    for c in ways("y"):
        pass_on("wo", 4, c, (2, 1))
    for c in ways("x"):
        if c not in EARLY_X:
            pass_on("wo", 2, c, (4, 1))

    settle(lambda kind, link: kind in ("wk", "wv"))
    half_rows = lambda n, r: pl.ds(pl.multiple_of(n * HALF + (dev(r) - 4 * mx) * ROWS, ROWS), ROWS)

    def half_load(n, r):
        c = ways("r")[n]
        src = wo_ref.at[:, chunk(c)] if r == 0 else place("wo", r, c)
        return pltpu.make_async_copy(src, wk_s.at[half_rows(n, r), :], tile_sem.at[c])

    def half_sum(rows, n, m):
        w = wk_s[pl.ds(n * HALF, HALF), pl.ds(pl.multiple_of(m * 256, 256), 256)]
        return _dot(rows, w, 1, 0)

    for n, c in enumerate(ways("r")):
        pass_on("wo", 2, c)
        wait_shared("wo", 1, c, wof_ref.at[pl.ds(0, 2 * ROWS), chunk(c)])
        for r in range(4):
            half_load(n, r).start()
    for n, c in enumerate(ways("r")):
        whole_tile = wk_s.at[pl.ds(n * HALF, HALF), :]
        pltpu.make_async_copy(whole_tile, whole_tile, tile_sem.at[c]).wait()

        def body(m, _):
            part_s[n, :, pl.ds(pl.multiple_of(m * 256, 256), 256)] = half_sum(give_s[...], n, m).astype(jnp.bfloat16)

        lax.fori_loop(0, WO[c][1] // 256, body, None)
        send("sum", 0, 4, c)

    rest(ahead, 6 * SG)
    for i in range(SG):
        finish(0, i, att_s, mx * HALF)

    for n, c in enumerate(ways("r")):

        def body(m, _):
            mine = att_s[:, pl.ds(pl.multiple_of(mx * HALF, HALF), HALF)]
            sum_s[n, :, pl.ds(pl.multiple_of(m * 256, 256), 256)] = half_sum(mine, n, m)

        lax.fori_loop(0, WO[c][1] // 256, body, None)

    for c in ways("x"):
        if c in FIRST_X:
            pass_on("wo", 4, c)
    for c in ways("y"):
        pass_on("wo", 2, c)
    settle(lambda kind, link: link == 1 or kind in ("wq", "x", "k", "v"))

    def tile(c):
        kind, at = TILES[c]
        return {"wq": wq_s, "wk": wk_s, "wv": wv_s}[kind], at

    def load(c, r):
        ref, at = tile(c)
        src = wo_ref.at[:, chunk(c)] if r == 0 else place("wo", r, c)
        return pltpu.make_async_copy(src, ref.at[wrows(r), pl.ds(at, WO[c][1])], tile_sem.at[c])

    def fetch(c):
        wait_shared("wo", 1, c, wof_ref.at[pl.ds(0, 3 * ROWS), chunk(c)])
        for r in range(6):
            load(c, r).start()

    def write(n):
        c = ORDER[n]
        return pltpu.make_async_copy(out_s.at[n % 2, :, pl.ds(0, WO[c][1])], y_ref.at[:, chunk(c)], out_sem.at[n % 2])

    def project(n, c):
        parts = 512 // WO[c][1]
        size = T // parts

        def body(m, _):
            rows = pl.ds(pl.multiple_of(m % parts * size, size), size)
            at = m // parts * 256
            cols = pl.ds(pl.multiple_of(at, 256), 256)
            if WO[c][2] == "r":
                i = ways("r").index(c)
                y = sum_s[i, rows, cols] + came_s[i, rows, cols].astype(jnp.float32)
            else:
                ref, left = tile(c)
                y = _dot(att_s[rows, :], ref[:, pl.ds(pl.multiple_of(left + at, 256), 256)], 1, 0)
            x = xo_s[rows, pl.ds(pl.multiple_of(WO[c][0] + at, 256), 256)].astype(jnp.float32)
            out_s[n % 2, rows, cols] = (x + y).astype(jnp.bfloat16)

        lax.fori_loop(0, 2, body, None)

    def complete(c):
        pass_on("wo", 6, c)
        load(c, 6).start()

    whole = tuple(c for c in ORDER if WO[c][2] != "r")
    after = {c: d for d in whole for c in whole if whole.index(c) < whole.index(d) and TILES[c] == TILES[d]}
    for c in whole:
        if c not in after.values():
            fetch(c)
    for i in range(SG):
        wait("att", 4, i)
    for what, c in STEPS:
        n = ORDER.index(c) if c in ORDER else None
        if what == "pass":
            complete(c)
        elif what == "load":
            wait("wo", 7, c)
            load(c, 7).start()
        else:
            if WO[c][2] == "r":
                wait("sum", 4, c)
            else:
                ref, at = tile(c)
                whole_tile = ref.at[:, pl.ds(at, WO[c][1])]
                pltpu.make_async_copy(whole_tile, whole_tile, tile_sem.at[c]).wait()
            if n >= 2:
                write(n - 2).wait()
            project(n, c)
            write(n).start()
            if c in after:
                fetch(after[c])
    for n in (len(ORDER) - 2, len(ORDER) - 1):
        write(n).wait()
    settle(lambda kind, link: True)


def _copy(part_ref, y_ref, y_s, in_sem, out_sem):
    rows = [pl.ds(n * T // PARTS, T // PARTS) for n in range(PARTS)]
    ins = [pltpu.make_async_copy(part_ref.at[at], y_s.at[at], in_sem.at[n]) for n, at in enumerate(rows)]
    outs = [pltpu.make_async_copy(y_s.at[at], y_ref.at[at], out_sem.at[n]) for n, at in enumerate(rows)]
    for copy in ins:
        copy.start()
    for n in range(PARTS):
        ins[n].wait()
        outs[n].start()
    for copy in outs:
        copy.wait()


PARTS = 8
RS = sum(way == "r" for _, _, way in WO)
SENDS = 42
RECVS = 61


def solution(mesh):
    freq = (THETA ** (-np.arange(HEAD // 2, dtype=np.float32) / (HEAD // 2))).astype(np.float32)
    freq = np.concatenate([freq, freq])[None]
    low = jnp.bfloat16
    vmem = pl.BlockSpec(memory_space=pltpu.VMEM)
    hbm = pl.BlockSpec(memory_space=pl.ANY)

    def step(x, gain, wq, wk, wv, wo):
        part, _ = pl.pallas_call(
            _kernel,
            name="half_layer",
            in_specs=[hbm, vmem, vmem, hbm, hbm, hbm, hbm],
            out_specs=[hbm, hbm],
            out_shape=[jax.ShapeDtypeStruct((T, D), low), jax.ShapeDtypeStruct((D, D), low)],
            scratch_shapes=[
                pltpu.VMEM((2, T, D), low),
                pltpu.VMEM((T, D), low),
                pltpu.VMEM((T, D), low),
                pltpu.VMEM((D, HALF), low),
                pltpu.VMEM((D, KW), low),
                pltpu.VMEM((D, KW), low),
                pltpu.VMEM((DEVICES, KH, T, HEAD), low),
                pltpu.VMEM((DEVICES, KH, HEAD, T), low),
                pltpu.VMEM((2, KH * G, T, HEAD), low),
                pltpu.VMEM((T, D), low),
                pltpu.VMEM((T, HALF), low),
                pltpu.VMEM((2, T, HEAD), jnp.float32),
                pltpu.VMEM((2, T, HEAD), jnp.float32),
                pltpu.VMEM((2, SG, 8, T), jnp.float32),
                pltpu.VMEM((2, SG, KH // SG * G, HEAD + 8, T), jnp.float32),
                pltpu.VMEM((2, T, 512), low),
                pltpu.VMEM((max(RS, 1), T, 512), jnp.float32),
                pltpu.VMEM((max(RS, 1), T, 512), low),
                pltpu.VMEM((max(RS, 1), T, 512), low),
                pltpu.SemaphoreType.DMA((SENDS,)),
                pltpu.SemaphoreType.DMA((RECVS,)),
                pltpu.SemaphoreType.DMA((5,)),
                pltpu.SemaphoreType.DMA((len(WO),)),
                pltpu.SemaphoreType.DMA((2,)),
            ],
            compiler_params=pltpu.CompilerParams(collective_id=0, has_side_effects=True, vmem_limit_bytes=67_000_000),
        )(x, gain, jnp.asarray(freq), wq, wk, wv, wo)
        return pl.pallas_call(
            _copy,
            name="result",
            in_specs=[hbm],
            out_specs=hbm,
            out_shape=jax.ShapeDtypeStruct((T, D), low),
            scratch_shapes=[pltpu.VMEM((T, D), low), pltpu.SemaphoreType.DMA((PARTS,)), pltpu.SemaphoreType.DMA((PARTS,))],
        )(part)

    tokens, whole = P(("dp", "sp"), None), P("sp", None)
    return jax.shard_map(
        step,
        mesh=mesh,
        in_specs=(tokens, P(None), whole, whole, whole, whole),
        out_specs=tokens,
        check_vma=False,
    )
```

```python
import jax
import jax.numpy as jnp
import numpy as np
from jax import lax
from jax.experimental import pallas as pl
from jax.experimental.pallas import tpu as pltpu
from jax.sharding import PartitionSpec as P

HEAD = 128
THETA = 10000
NEG = -1e30
HIDDEN = 2 * NEG
LOG2E = 1.4426950408889634
MESH = pl.DeviceIdType.MESH
DEVICES = 8

T = 512
D = 3072
ROWS = D // DEVICES
HALF = D // 2
KH = 4
KW = KH * HEAD
G = 3
SG = 2
SGW = HALF // SG
WO = ((0, 512, "y"), (512, 512, "y"), (1024, 256, "y"), (1280, 256, "y"), (1536, 256, "x"), (1792, 256, "x"), (2048, 512, "r"), (2560, 512, "r"))
TILES = {0: ("wq", 0), 1: ("wq", 512), 4: ("wq", 1024), 5: ("wq", 1280), 2: ("wv", 0), 3: ("wv", 256)}
EARLY_X = (4, 5)
FINAL = 3
FIRST_X = (0, 1, 2, 3, 4, 5)
FIRST_Y = (4, 5, 2)
STEPS = (("pass", 4), ("pass", 5), ("load", 4), ("load", 5), ("done", 4), ("done", 5), ("most", 3), ("pass", 0), ("load", 0), ("done", 0), ("pass", 1), ("load", 1), ("done", 6), ("done", 1), ("pass", 2), ("load", 2), ("pass", 3), ("done", 2), ("done", 7))
ORDER = (4, 5, 0, 6, 1, 2, 7)


def _dot(a, b, ca, cb):
    return lax.dot_general(a, b, (((ca,), (cb,)), ((), ())), preferred_element_type=jnp.float32)


def _kernel(
    x_ref, gain_ref, freq_ref, wq_ref, wk_ref, wv_ref, wo_ref,
    y_ref, wof_ref, most_ref, far_ref,
    a_s, xo_s, xr_s, wq_s, wk_s, wv_s, k_s, v_s, q_s, att_s, give_s, cos_s, sin_s, top_s, mix_s, out_s, sum_s, part_s, came_s, most_s,
    send_sem, recv_sem, local_sem, tile_sem, out_sem,
):
    me = lax.axis_index("sp")
    mx, my, mk = me // 4, (me // 2) % 2, me % 2

    def dev(r):
        x = 1 - mx if r & 4 else mx
        y = 1 - my if r & 2 else my
        k = 1 - mk if r & 1 else mk
        return 4 * x + 2 * y + k

    def wrows(r):
        return pl.ds(pl.multiple_of(dev(r) * ROWS, ROWS), ROWS)

    def half(h, width):
        return pl.ds(pl.multiple_of(h * width, width), width)

    def chunk(c):
        return pl.ds(WO[c][0], WO[c][1])

    def ways(*which):
        return tuple(c for c in range(len(WO)) if WO[c][2] in which)

    def place(kind, r, i):
        if kind == "wk":
            return wk_s.at[wrows(r)]
        if kind == "wv":
            return wv_s.at[wrows(r)]
        if kind == "wq":
            return wq_s.at[wrows(r), pl.ds(i * SGW, SGW)]
        if kind == "k":
            return k_s.at[dev(r)]
        if kind == "v":
            return v_s.at[dev(r)]
        if kind == "wo":
            return wof_ref.at[wrows(r), chunk(i)]
        if kind == "x":
            return xr_s
        if kind == "att":
            return give_s.at[:, pl.ds(i * SGW, SGW)]
        if kind == "sum":
            return part_s.at[ways("r").index(i)]

    def own(kind, h, i):
        if kind == "wk":
            return wk_ref.at[:, half(h, KW)]
        if kind == "wv":
            return wv_ref.at[:, half(h, KW)]
        if kind == "wq":
            return wq_ref.at[:, pl.ds(pl.multiple_of(h * HALF + i * SGW, SGW), SGW)]
        if kind == "wo":
            return wo_ref.at[:, chunk(i)]
        if kind == "x":
            return x_ref
        return place(kind, 0, i)

    recv_index = {}

    def recv(kind, r, i):
        key = (kind, r, i)
        if r % 2 and kind in ("wk", "wv"):
            key = ("w", 1, 0)
        elif r % 2 and kind == "wq":
            key = ("wq", 1, i)
        elif r % 2 and kind in ("k", "v"):
            key = ("kv", {1: 1, 3: 3, 5: 3, 7: 7}[r], 0)
        elif r in (1, 3, 5) and kind == "wo":
            key = ("wo", 1, i)
        return recv_sem.at[recv_index.setdefault(key, len(recv_index))]

    def wait_shared(kind, r, i, like):
        sem = recv(kind, r, i)
        pltpu.make_async_remote_copy(
            src_ref=like, dst_ref=like, send_sem=send_sem.at[0], recv_sem=sem, device_id={"sp": dev(4)}, device_id_type=MESH
        ).wait_recv()

    taken = []
    started, settled, free = [], [], list(range(SENDS))

    def settle(which):
        for n, (kind, link, copy) in enumerate(started):
            if n not in settled and which(kind, link):
                copy.wait_send()
                settled.append(n)
                free.append(taken[n])

    def send(kind, r, link, i=0):
        src = own(kind, 1 - mx if link == 4 else mx, i) if r == 0 else place(kind, r, i)
        if kind == "att":
            dst = att_s.at[:, pl.ds(pl.multiple_of(mx * HALF + i * SGW, SGW), SGW)]
        elif kind == "sum":
            dst = came_s.at[ways("r").index(i)]
        else:
            dst = place(kind, r, i)
        taken.append(free.pop(free.index(min(free))))
        copy = pltpu.make_async_remote_copy(
            src_ref=src, dst_ref=dst, send_sem=send_sem.at[taken[-1]], recv_sem=recv(kind, r ^ link, i),
            device_id={"sp": dev(link)}, device_id_type=MESH,
        )
        copy.start()
        started.append((kind, link, copy))

    def wait(kind, r, i=0):
        if kind == "att":
            dst = att_s.at[:, pl.ds(pl.multiple_of((1 - mx) * HALF + i * SGW, SGW), SGW)]
        elif kind == "sum":
            dst = came_s.at[ways("r").index(i)]
        else:
            dst = place(kind, r, i)
        pltpu.make_async_remote_copy(
            src_ref=dst, dst_ref=dst, send_sem=send_sem.at[0], recv_sem=recv(kind, r, i),
            device_id={"sp": dev(4)}, device_id_type=MESH,
        ).wait_recv()

    barrier = pltpu.get_barrier_semaphore()
    for link in (1, 2, 4):
        pl.semaphore_signal(barrier, 1, device_id={"sp": dev(link)}, device_id_type=MESH)
    pl.semaphore_wait(barrier, 3)

    for kind in ("wk", "wv"):
        send(kind, 0, 4)
        send(kind, 0, 2)
    for i in range(SG):
        send("wq", 0, 4, i)
    send("wq", 0, 2, 0)
    send("x", 0, 4)
    for c in FIRST_X:
        send("wo", 0, 4, c)
    local = [
        pltpu.make_async_copy(x_ref, xo_s, local_sem.at[0]),
        pltpu.make_async_copy(own("wk", mx, 0), place("wk", 0, 0), local_sem.at[1]),
        pltpu.make_async_copy(own("wv", mx, 0), place("wv", 0, 0), local_sem.at[2]),
        pltpu.make_async_copy(own("wq", mx, 0), place("wq", 0, 0), local_sem.at[3]),
        pltpu.make_async_copy(own("wq", mx, 1), place("wq", 0, 1), local_sem.at[4]),
    ]
    for copy in local:
        copy.start()
    for kind in ("wk", "wv"):
        send(kind, 0, 1)
    for i in range(SG):
        send("wq", 0, 1, i)

    def tables(t, block):
        def body(i, _):
            at = pl.ds(pl.multiple_of(i * 64, 64), 64)
            token = block * T + i * 64 + lax.broadcasted_iota(jnp.int32, (64, HEAD), 0)
            angle = token.astype(jnp.float32) * freq_ref[...]
            cos_s[t, at, :] = jnp.cos(angle)
            sin = jnp.sin(angle)
            lane = lax.broadcasted_iota(jnp.int32, (64, HEAD), 1)
            sin_s[t, at, :] = jnp.where(lane < HEAD // 2, -sin, sin)

        lax.fori_loop(0, T // 64, body, None)

    def norm(src, t):
        def body(i, _):
            at = pl.ds(pl.multiple_of(i * 32, 32), 32)
            wide = src[at, :].astype(jnp.float32)
            scale = lax.rsqrt(jnp.mean(wide * wide, -1, keepdims=True) + 1e-6)
            a_s[t, at, :] = (wide * scale * gain_ref[...].astype(jnp.float32)[None]).astype(jnp.bfloat16)

        lax.fori_loop(0, T // 32, body, None)

    def turned(t, value):
        wide = value.astype(jnp.bfloat16).astype(jnp.float32)
        return (wide * cos_s[t] + pltpu.roll(wide, HEAD // 2, 1) * sin_s[t]).astype(jnp.bfloat16)

    def keys_values(t, block):
        def body(n, _):
            cols = pl.ds(pl.multiple_of(n * 256, 256), 256)
            k = _dot(a_s[t], wk_s[:, cols], 1, 0)
            v = _dot(a_s[t], wv_s[:, cols], 1, 0).astype(jnp.bfloat16)
            for h in range(2):
                lanes = slice(h * HEAD, (h + 1) * HEAD)
                k_s[block, 2 * n + h] = turned(t, k[:, lanes])
                v_s[block, 2 * n + h] = v[:, lanes].T

        lax.fori_loop(0, KW // 256, body, None)

    def queries(t, i):
        def body(n, _):
            cols = pl.ds(pl.multiple_of(i * SGW + n * 256, 256), 256)
            q = _dot(a_s[t], wq_s[:, cols], 1, 0)
            for h in range(2):
                q_s[t, i * (SGW // HEAD) + 2 * n + h] = turned(t, q[:, h * HEAD : (h + 1) * HEAD])

        lax.fori_loop(0, SGW // 256, body, None)

    local[0].wait()
    tables(0, me)
    norm(xo_s, 0)
    tables(1, dev(4))

    def pass_on(kind, r, i=0, links=(1,)):
        wait(kind, r, i)
        for link in links:
            send(kind, r, link, i)

    both = ("wk", "wv")
    for kind in both:
        pass_on(kind, 4, 0, (2, 1))
    pass_on("wq", 4, 0, (2, 1))
    send("wq", 0, 2, 1)
    pass_on("wq", 4, 1, (2, 1))
    for kind in both:
        pass_on(kind, 2)
    for kind in both:
        pass_on(kind, 6)
    wait_shared("wk", 1, 0, wk_s)
    settle(lambda kind, link: link == 1)
    for copy in local[1:3]:
        copy.wait()

    keys_values(0, me)
    for kind in ("k", "v"):
        send(kind, 0, 2)
        send(kind, 0, 1)
    for c in FIRST_Y:
        send("wo", 0, 2, c)
    for c in range(len(WO)):
        send("wo", 0, 1, c)

    def whole_wq(i):
        pass_on("wq", 6, i)
        wait_shared("wq", 1, i, wq_s.at[pl.ds(0, D // 2), pl.ds(i * SGW, SGW)])
        local[3 + i].wait()

    def whole_wq(i):
        pass_on("wq", 6, i)
        wait_shared("wq", 1, i, wq_s.at[pl.ds(0, D // 2), pl.ds(i * SGW, SGW)])
        local[3 + i].wait()

    e = HEAD**-0.5 * LOG2E
    ones = jnp.ones((8, T), jnp.bfloat16)
    per = KH // SG
    pieces = [(kv, n) for kv in range(per) for n in range(G)]
    mine = (me, dev(4))

    def begin():
        top_s[...] = jnp.full(top_s.shape, NEG, jnp.float32)

        def body(n, _):
            mix_s[n // SG, n % SG] = jnp.zeros(mix_s.shape[2:], jnp.float32)

        lax.fori_loop(0, 2 * SG, body, None)

    def step(t, i, j, masked):
        scores = [_dot(k_s[j, i * per + kv], q_s[t, (i * per + kv) * G + n], 1, 1) for kv, n in pieces]
        if masked:
            ok = lax.broadcasted_iota(jnp.int32, (T, T), 0) <= lax.broadcasted_iota(jnp.int32, (T, T), 1)
        weights, keeps = [], []
        for p, s in enumerate(scores):
            if masked:
                s = jnp.where(ok, s, HIDDEN)
            old = top_s[t, i, p : p + 1, :]
            top = jnp.maximum(old, s.max(axis=0, keepdims=True))
            top_s[t, i, p : p + 1, :] = top
            weights.append(jnp.exp2((s - top) * e).astype(jnp.bfloat16))
            keeps.append(jnp.exp2((old - top) * e))
        for p, (kv, n) in enumerate(pieces):
            values = jnp.concatenate([v_s[j, i * per + kv], ones], axis=0)
            mix_s[t, i, p] = mix_s[t, i, p] * keeps[p] + _dot(values, weights[p], 1, 0)

    def last(t):
        return me + t * (dev(4) - me)

    def some(r):
        x, y, k = r // 4, (r // 2) % 2, r % 2
        return 4 * (mx + x - 2 * mx * x) + 2 * (my + y - 2 * my * y) + mk + k - 2 * mk * k

    def over(first, count, item):
        def body(n, _):
            t, i, r = item(n)

            @pl.when(some(r) < last(t))
            def _():
                step(t, i, some(r), False)

        lax.fori_loop(first, count, body, None)

    def diagonal(t):
        lax.fori_loop(0, SG, lambda i, _: step(t, i, mine[t], True), None)

    def finish(t, i, out, base):
        for p in range(len(pieces)):
            total = mix_s[t, i, p, HEAD : HEAD + 1, :]
            at = pl.multiple_of(base + i * SGW + p * HEAD, HEAD)
            out[:, pl.ds(at, HEAD)] = (mix_s[t, i, p, :HEAD, :] * (1 / total)).T.astype(jnp.bfloat16)

    def near():
        begin()
        diagonal(0)
        over(0, SG, lambda n: (0, n, 1))

    def early(first, count):
        over(first, count, lambda n: (1, n // 5, (5 + n % 5) % 6))

    def late(i):
        over(6, 8, lambda n: (1, i, n))
        finish(1, i, give_s, 0)

    def rest(first, count):
        over(first, count, lambda n: (0, n % SG, 2 + n // SG))

    ahead = 2 * SG * mx

    for i in range(SG):
        pass_on("wq", 2, i)
        whole_wq(i)
        queries(0, i)
    wait_shared("k", 1, 0, k_s.at[pl.ds(0, 2)])
    near()
    settle(lambda kind, link: kind in ("wk", "wv", "wq"))
    wait("x", 4)
    norm(xr_s, 1)
    keys_values(1, dev(4))
    for kind in ("k", "v"):
        send(kind, 4, 2)
        send(kind, 4, 1)
    for c in ways("r") + ways("y"):
        if c not in FIRST_Y:
            send("wo", 0, 2, c)
    for kind in ("k", "v"):
        pass_on(kind, 2)
    for c in EARLY_X:
        pass_on("wo", 2, c, (4, 1))
    for i in range(SG):
        queries(1, i)
    wait_shared("k", 3, 0, k_s.at[pl.ds(0, 4)])
    settle(lambda kind, link: link == 1 or kind == "x")
    diagonal(1)
    early(0, 7)
    rest(0, ahead)
    for kind in ("k", "v"):
        pass_on(kind, 6)
    wait_shared("k", 7, 0, k_s.at[pl.ds(0, 2)])
    late(0)
    send("att", 0, 4, 0)
    early(7, 10)
    late(1)
    send("att", 0, 4, 1)
    for c in ways("y", "x"):
        if c not in FIRST_X:
            send("wo", 0, 4, c)
    for c in ways("y"):
        pass_on("wo", 4, c, (2, 1))
    for c in ways("x"):
        if c not in EARLY_X:
            pass_on("wo", 2, c, (4, 1))

    settle(lambda kind, link: kind in ("wk", "wv"))
    half_rows = lambda n, r: pl.ds(pl.multiple_of(n * HALF + (dev(r) - 4 * mx) * ROWS, ROWS), ROWS)

    def half_load(n, r):
        c = ways("r")[n]
        src = wo_ref.at[:, chunk(c)] if r == 0 else place("wo", r, c)
        return pltpu.make_async_copy(src, wk_s.at[half_rows(n, r), :], tile_sem.at[c])

    def half_sum(rows, n, m):
        w = wk_s[pl.ds(n * HALF, HALF), pl.ds(pl.multiple_of(m * 256, 256), 256)]
        return _dot(rows, w, 1, 0)

    for n, c in enumerate(ways("r")):
        pass_on("wo", 2, c)
        wait_shared("wo", 1, c, wof_ref.at[pl.ds(0, 2 * ROWS), chunk(c)])
        for r in range(4):
            half_load(n, r).start()
    for n, c in enumerate(ways("r")):
        whole_tile = wk_s.at[pl.ds(n * HALF, HALF), :]
        pltpu.make_async_copy(whole_tile, whole_tile, tile_sem.at[c]).wait()

        def body(m, _):
            part_s[n, :, pl.ds(pl.multiple_of(m * 256, 256), 256)] = half_sum(give_s[...], n, m).astype(jnp.bfloat16)

        lax.fori_loop(0, WO[c][1] // 256, body, None)
        send("sum", 0, 4, c)

    rest(ahead, 6 * SG)
    for i in range(SG):
        finish(0, i, att_s, mx * HALF)

    for n, c in enumerate(ways("r")):

        def body(m, _):
            mine = att_s[:, pl.ds(pl.multiple_of(mx * HALF, HALF), HALF)]
            sum_s[n, :, pl.ds(pl.multiple_of(m * 256, 256), 256)] = half_sum(mine, n, m)

        lax.fori_loop(0, WO[c][1] // 256, body, None)

    for c in ways("x"):
        if c in FIRST_X:
            pass_on("wo", 4, c)
    for c in ways("y"):
        pass_on("wo", 2, c)
    settle(lambda kind, link: link == 1 or kind in ("wq", "x", "k", "v"))

    def tile(c):
        kind, at = TILES[c]
        return {"wq": wq_s, "wk": wk_s, "wv": wv_s}[kind], at

    def load(c, r):
        ref, at = tile(c)
        src = wo_ref.at[:, chunk(c)] if r == 0 else place("wo", r, c)
        return pltpu.make_async_copy(src, ref.at[wrows(r), pl.ds(at, WO[c][1])], tile_sem.at[c])

    def fetch(c):
        wait_shared("wo", 1, c, wof_ref.at[pl.ds(0, 3 * ROWS), chunk(c)])
        for r in range(6):
            load(c, r).start()

    def write(n):
        c = ORDER[n]
        return pltpu.make_async_copy(out_s.at[n % 2, :, pl.ds(0, WO[c][1])], y_ref.at[:, chunk(c)], out_sem.at[n % 2])

    def project(n, c):
        parts = 512 // WO[c][1]
        size = T // parts

        def body(m, _):
            rows = pl.ds(pl.multiple_of(m % parts * size, size), size)
            at = m // parts * 256
            cols = pl.ds(pl.multiple_of(at, 256), 256)
            if WO[c][2] == "r":
                i = ways("r").index(c)
                y = sum_s[i, rows, cols] + came_s[i, rows, cols].astype(jnp.float32)
            else:
                ref, left = tile(c)
                y = _dot(att_s[rows, :], ref[:, pl.ds(pl.multiple_of(left + at, 256), 256)], 1, 0)
            x = xo_s[rows, pl.ds(pl.multiple_of(WO[c][0] + at, 256), 256)].astype(jnp.float32)
            out_s[n % 2, rows, cols] = (x + y).astype(jnp.bfloat16)

        lax.fori_loop(0, 2, body, None)

    def complete(c):
        pass_on("wo", 6, c)
        if c != FINAL:
            load(c, 6).start()

    far = (2 - 2 * mx) + (1 - my)
    FAR = 2 * ROWS

    def most():
        ref, left = tile(FINAL)
        start, width, _ = WO[FINAL]
        got = ref.at[pl.ds(0, D - FAR), pl.ds(left, width)]
        pltpu.make_async_copy(got, got, tile_sem.at[FINAL]).wait()

        def body(m, _):
            rows = pl.ds(pl.multiple_of(m * 256, 256), 256)
            y = xo_s[rows, pl.ds(start, width)].astype(jnp.float32)
            for n in range(1, 4):
                at = pl.ds(pl.multiple_of((far + n) % 4 * FAR, FAR), FAR)
                y += _dot(att_s[rows, at], ref[at, pl.ds(left, width)], 1, 0)
            most_s[rows, :] = y

        lax.fori_loop(0, T // 256, body, None)
        for copy in kept:
            copy.start()

    kept = [
        pltpu.make_async_copy(most_s, most_ref, local_sem.at[0]),
        pltpu.make_async_copy(att_s.at[:, pl.ds(pl.multiple_of(far * FAR, FAR), FAR)], far_ref, local_sem.at[1]),
    ]

    whole = tuple(c for c in ORDER + (FINAL,) if WO[c][2] != "r")
    after = {c: d for d in whole for c in whole if whole.index(c) < whole.index(d) and TILES[c] == TILES[d]}
    for c in whole:
        if c not in after.values():
            fetch(c)
    for i in range(SG):
        wait("att", 4, i)
    for what, c in STEPS:
        n = ORDER.index(c) if c in ORDER else None
        if what == "pass":
            complete(c)
        elif what == "most":
            most()
        elif what == "load":
            wait("wo", 7, c)
            load(c, 7).start()
        else:
            if WO[c][2] == "r":
                wait("sum", 4, c)
            else:
                ref, at = tile(c)
                whole_tile = ref.at[:, pl.ds(at, WO[c][1])]
                pltpu.make_async_copy(whole_tile, whole_tile, tile_sem.at[c]).wait()
            if n >= 2:
                write(n - 2).wait()
            project(n, c)
            write(n).start()
            if c in after:
                fetch(after[c])
    wait("wo", 7, FINAL)
    for copy in kept:
        copy.wait()
    for n in (len(ORDER) - 2, len(ORDER) - 1):
        write(n).wait()
    settle(lambda kind, link: True)


def _end(part_ref, most_ref, far_ref, wof_ref, y_ref, y_s, most_s, far_s, w_s, in_sem, out_sem):
    me = lax.axis_index("sp")
    start, width, _ = WO[FINAL]
    cols = pl.ds(start, width)
    rows = pl.ds(pl.multiple_of(((2 - me // 4 * 2) + (1 - me // 2 % 2)) * 2 * ROWS, 2 * ROWS), 2 * ROWS)
    first = [
        pltpu.make_async_copy(wof_ref.at[rows, cols], w_s, in_sem.at[PARTS]),
        pltpu.make_async_copy(far_ref, far_s, in_sem.at[PARTS + 1]),
        pltpu.make_async_copy(most_ref, most_s, in_sem.at[PARTS + 2]),
    ]
    size = 2 * T // PARTS
    ways = [(pl.ds(n // 2 * size, size), (pl.ds(0, start), pl.ds(start + width, D - start - width))[n % 2]) for n in range(PARTS)]
    ins = [pltpu.make_async_copy(part_ref.at[at], y_s.at[at], in_sem.at[n]) for n, at in enumerate(ways)]
    outs = [pltpu.make_async_copy(y_s.at[at], y_ref.at[at], out_sem.at[n]) for n, at in enumerate(ways + [(slice(None), cols)])]
    for copy in first + ins:
        copy.start()
    for copy in first:
        copy.wait()
    y_s[:, cols] = (most_s[...] + _dot(far_s[...], w_s[...], 1, 0)).astype(jnp.bfloat16)
    for n in range(PARTS):
        ins[n].wait()
        outs[n].start()
    outs[PARTS].start()
    for copy in outs:
        copy.wait()


PARTS = 8
RS = sum(way == "r" for _, _, way in WO)
SENDS = 42
RECVS = 61


def solution(mesh):
    freq = (THETA ** (-np.arange(HEAD // 2, dtype=np.float32) / (HEAD // 2))).astype(np.float32)
    freq = np.concatenate([freq, freq])[None]
    low = jnp.bfloat16
    vmem = pl.BlockSpec(memory_space=pltpu.VMEM)
    hbm = pl.BlockSpec(memory_space=pl.ANY)

    def step(x, gain, wq, wk, wv, wo):
        part, gathered, most, far = pl.pallas_call(
            _kernel,
            name="half_layer",
            in_specs=[hbm, vmem, vmem, hbm, hbm, hbm, hbm],
            out_specs=[hbm] * 4,
            out_shape=[
                jax.ShapeDtypeStruct((T, D), low),
                jax.ShapeDtypeStruct((D, D), low),
                jax.ShapeDtypeStruct((T, WO[FINAL][1]), jnp.float32),
                jax.ShapeDtypeStruct((T, 2 * ROWS), low),
            ],
            scratch_shapes=[
                pltpu.VMEM((2, T, D), low),
                pltpu.VMEM((T, D), low),
                pltpu.VMEM((T, D), low),
                pltpu.VMEM((D, HALF), low),
                pltpu.VMEM((D, KW), low),
                pltpu.VMEM((D, KW), low),
                pltpu.VMEM((DEVICES, KH, T, HEAD), low),
                pltpu.VMEM((DEVICES, KH, HEAD, T), low),
                pltpu.VMEM((2, KH * G, T, HEAD), low),
                pltpu.VMEM((T, D), low),
                pltpu.VMEM((T, HALF), low),
                pltpu.VMEM((2, T, HEAD), jnp.float32),
                pltpu.VMEM((2, T, HEAD), jnp.float32),
                pltpu.VMEM((2, SG, 8, T), jnp.float32),
                pltpu.VMEM((2, SG, KH // SG * G, HEAD + 8, T), jnp.float32),
                pltpu.VMEM((2, T, 512), low),
                pltpu.VMEM((max(RS, 1), T, 512), jnp.float32),
                pltpu.VMEM((max(RS, 1), T, 512), low),
                pltpu.VMEM((max(RS, 1), T, 512), low),
                pltpu.VMEM((T, WO[FINAL][1]), jnp.float32),
                pltpu.SemaphoreType.DMA((SENDS,)),
                pltpu.SemaphoreType.DMA((RECVS,)),
                pltpu.SemaphoreType.DMA((5,)),
                pltpu.SemaphoreType.DMA((len(WO),)),
                pltpu.SemaphoreType.DMA((2,)),
            ],
            compiler_params=pltpu.CompilerParams(collective_id=0, has_side_effects=True, vmem_limit_bytes=67_000_000),
        )(x, gain, jnp.asarray(freq), wq, wk, wv, wo)
        return pl.pallas_call(
            _end,
            name="end",
            in_specs=[hbm] * 4,
            out_specs=hbm,
            out_shape=jax.ShapeDtypeStruct((T, D), low),
            scratch_shapes=[
                pltpu.VMEM((T, D), low),
                pltpu.VMEM((T, WO[FINAL][1]), jnp.float32),
                pltpu.VMEM((T, 2 * ROWS), low),
                pltpu.VMEM((2 * ROWS, WO[FINAL][1]), low),
                pltpu.SemaphoreType.DMA((PARTS + 3,)),
                pltpu.SemaphoreType.DMA((PARTS + 1,)),
            ],
        )(part, most, far, gathered)

    tokens, whole = P(("dp", "sp"), None), P("sp", None)
    return jax.shard_map(
        step,
        mesh=mesh,
        in_specs=(tokens, P(None), whole, whole, whole, whole),
        out_specs=tokens,
        check_vma=False,
    )
```

```python
import jax
import jax.numpy as jnp
import numpy as np
from jax import lax
from jax.experimental import pallas as pl
from jax.experimental.pallas import tpu as pltpu
from jax.sharding import PartitionSpec as P

HEAD = 128
THETA = 10000
NEG = -1e30
HIDDEN = 2 * NEG
LOG2E = 1.4426950408889634
MESH = pl.DeviceIdType.MESH
DEVICES = 8

T = 512
D = 3072
ROWS = D // DEVICES
HALF = D // 2
KH = 4
KW = KH * HEAD
G = 3
SG = 2
SGW = HALF // SG
WIDTHS = ((512, "y"), (512, "y"), (256, "y"), (256, "y"), (256, "x"), (256, "x"), (512, "r"), (512, "r"))
WO = tuple((sum(w for w, _ in WIDTHS[:n]), *chunk) for n, chunk in enumerate(WIDTHS))
TILES = {0: ("wq", 0), 1: ("wq", 512), 4: ("wq", 1024), 5: ("wq", 1280), 2: ("wv", 0), 3: ("wv", 256)}
EARLY_X = (4, 5)
FINAL = 3
FIRST_X = tuple(range(6))
FIRST_Y = (4, 5, 2)
STEPS = (("pass", 4), ("pass", 5), ("load", 4), ("load", 5), ("done", 4), ("done", 5), ("most", 3), ("pass", 0), ("load", 0), ("done", 0), ("pass", 1), ("load", 1), ("done", 6), ("done", 1), ("pass", 2), ("load", 2), ("pass", 3), ("done", 2), ("done", 7))
ORDER = tuple(c for what, c in STEPS if what == "done")


def _dot(a, b, ca, cb):
    return lax.dot_general(a, b, (((ca,), (cb,)), ((), ())), preferred_element_type=jnp.float32)


def _kernel(
    x_ref, gain_ref, freq_ref, wq_ref, wk_ref, wv_ref, wo_ref,
    y_ref, wof_ref, most_ref, far_ref,
    a_s, xo_s, xr_s, wq_s, wk_s, wv_s, k_s, v_s, q_s, att_s, give_s, cos_s, sin_s, top_s, mix_s, out_s, sum_s, part_s, came_s, most_s,
    send_sem, recv_sem, local_sem, tile_sem, out_sem,
):
    me = lax.axis_index("sp")
    mx, my, mk = me // 4, (me // 2) % 2, me % 2

    def dev(r):
        x = 1 - mx if r & 4 else mx
        y = 1 - my if r & 2 else my
        k = 1 - mk if r & 1 else mk
        return 4 * x + 2 * y + k

    def wrows(r):
        return pl.ds(pl.multiple_of(dev(r) * ROWS, ROWS), ROWS)

    def half(h, width):
        return pl.ds(pl.multiple_of(h * width, width), width)

    def chunk(c):
        return pl.ds(WO[c][0], WO[c][1])

    def ways(*which):
        return tuple(c for c in range(len(WO)) if WO[c][2] in which)

    def place(kind, r, i):
        if kind == "wk":
            return wk_s.at[wrows(r)]
        if kind == "wv":
            return wv_s.at[wrows(r)]
        if kind == "wq":
            return wq_s.at[wrows(r), pl.ds(i * SGW, SGW)]
        if kind == "k":
            return k_s.at[dev(r)]
        if kind == "v":
            return v_s.at[dev(r)]
        if kind == "wo":
            return wof_ref.at[wrows(r), chunk(i)]
        if kind == "x":
            return xr_s
        if kind == "att":
            return give_s.at[:, pl.ds(i * SGW, SGW)]
        if kind == "sum":
            return part_s.at[ways("r").index(i)]

    def own(kind, h, i):
        if kind == "wk":
            return wk_ref.at[:, half(h, KW)]
        if kind == "wv":
            return wv_ref.at[:, half(h, KW)]
        if kind == "wq":
            return wq_ref.at[:, pl.ds(pl.multiple_of(h * HALF + i * SGW, SGW), SGW)]
        if kind == "wo":
            return wo_ref.at[:, chunk(i)]
        if kind == "x":
            return x_ref
        return place(kind, 0, i)

    recv_index = {}

    def recv(kind, r, i):
        key = (kind, r, i)
        if r % 2 and kind in ("wk", "wv"):
            key = ("w", 1, 0)
        elif r % 2 and kind == "wq":
            key = ("wq", 1, i)
        elif r % 2 and kind in ("k", "v"):
            key = ("kv", 3 if r == 5 else r, 0)
        elif r in (1, 3, 5) and kind == "wo":
            key = ("wo", 1, i)
        return recv_sem.at[recv_index.setdefault(key, len(recv_index))]

    def wait_shared(kind, r, i, like):
        sem = recv(kind, r, i)
        pltpu.make_async_remote_copy(
            src_ref=like, dst_ref=like, send_sem=send_sem.at[0], recv_sem=sem, device_id={"sp": dev(4)}, device_id_type=MESH
        ).wait_recv()

    taken = []
    started, settled, free = [], [], list(range(SENDS))

    def settle(which):
        for n, (kind, link, copy) in enumerate(started):
            if n not in settled and which(kind, link):
                copy.wait_send()
                settled.append(n)
                free.append(taken[n])

    def send(kind, r, link, i=0):
        src = own(kind, 1 - mx if link == 4 else mx, i) if r == 0 else place(kind, r, i)
        if kind == "att":
            dst = att_s.at[:, pl.ds(pl.multiple_of(mx * HALF + i * SGW, SGW), SGW)]
        elif kind == "sum":
            dst = came_s.at[ways("r").index(i)]
        else:
            dst = place(kind, r, i)
        taken.append(free.pop(free.index(min(free))))
        copy = pltpu.make_async_remote_copy(
            src_ref=src, dst_ref=dst, send_sem=send_sem.at[taken[-1]], recv_sem=recv(kind, r ^ link, i),
            device_id={"sp": dev(link)}, device_id_type=MESH,
        )
        copy.start()
        started.append((kind, link, copy))

    def wait(kind, r, i=0):
        if kind == "att":
            dst = att_s.at[:, pl.ds(pl.multiple_of((1 - mx) * HALF + i * SGW, SGW), SGW)]
        elif kind == "sum":
            dst = came_s.at[ways("r").index(i)]
        else:
            dst = place(kind, r, i)
        pltpu.make_async_remote_copy(
            src_ref=dst, dst_ref=dst, send_sem=send_sem.at[0], recv_sem=recv(kind, r, i),
            device_id={"sp": dev(4)}, device_id_type=MESH,
        ).wait_recv()

    barrier = pltpu.get_barrier_semaphore()
    for link in (1, 2, 4):
        pl.semaphore_signal(barrier, 1, device_id={"sp": dev(link)}, device_id_type=MESH)
    pl.semaphore_wait(barrier, 3)

    for kind in ("wk", "wv"):
        send(kind, 0, 4)
        send(kind, 0, 2)
    for i in range(SG):
        send("wq", 0, 4, i)
    send("wq", 0, 2, 0)
    send("x", 0, 4)
    for c in FIRST_X:
        send("wo", 0, 4, c)
    local = [
        pltpu.make_async_copy(x_ref, xo_s, local_sem.at[0]),
        pltpu.make_async_copy(own("wk", mx, 0), place("wk", 0, 0), local_sem.at[1]),
        pltpu.make_async_copy(own("wv", mx, 0), place("wv", 0, 0), local_sem.at[2]),
        pltpu.make_async_copy(own("wq", mx, 0), place("wq", 0, 0), local_sem.at[3]),
        pltpu.make_async_copy(own("wq", mx, 1), place("wq", 0, 1), local_sem.at[4]),
    ]
    for copy in local:
        copy.start()
    for kind in ("wk", "wv"):
        send(kind, 0, 1)
    for i in range(SG):
        send("wq", 0, 1, i)

    def tables(t, block):
        def body(i, _):
            at = pl.ds(pl.multiple_of(i * 64, 64), 64)
            token = block * T + i * 64 + lax.broadcasted_iota(jnp.int32, (64, HEAD), 0)
            angle = token.astype(jnp.float32) * freq_ref[...]
            cos_s[t, at, :] = jnp.cos(angle)
            sin = jnp.sin(angle)
            lane = lax.broadcasted_iota(jnp.int32, (64, HEAD), 1)
            sin_s[t, at, :] = jnp.where(lane < HEAD // 2, -sin, sin)

        lax.fori_loop(0, T // 64, body, None)

    def norm(src, t):
        def body(i, _):
            at = pl.ds(pl.multiple_of(i * 32, 32), 32)
            wide = src[at, :].astype(jnp.float32)
            scale = lax.rsqrt(jnp.mean(wide * wide, -1, keepdims=True) + 1e-6)
            a_s[t, at, :] = (wide * scale * gain_ref[...].astype(jnp.float32)[None]).astype(jnp.bfloat16)

        lax.fori_loop(0, T // 32, body, None)

    def turned(t, value):
        wide = value.astype(jnp.bfloat16).astype(jnp.float32)
        return (wide * cos_s[t] + pltpu.roll(wide, HEAD // 2, 1) * sin_s[t]).astype(jnp.bfloat16)

    def keys_values(t, block):
        def body(n, _):
            cols = pl.ds(pl.multiple_of(n * 256, 256), 256)
            k = _dot(a_s[t], wk_s[:, cols], 1, 0)
            v = _dot(a_s[t], wv_s[:, cols], 1, 0).astype(jnp.bfloat16)
            for h in range(2):
                lanes = slice(h * HEAD, (h + 1) * HEAD)
                k_s[block, 2 * n + h] = turned(t, k[:, lanes])
                v_s[block, 2 * n + h] = v[:, lanes].T

        lax.fori_loop(0, KW // 256, body, None)

    def queries(t, i):
        def body(n, _):
            cols = pl.ds(pl.multiple_of(i * SGW + n * 256, 256), 256)
            q = _dot(a_s[t], wq_s[:, cols], 1, 0)
            for h in range(2):
                q_s[t, i * (SGW // HEAD) + 2 * n + h] = turned(t, q[:, h * HEAD : (h + 1) * HEAD])

        lax.fori_loop(0, SGW // 256, body, None)

    local[0].wait()
    tables(0, me)
    norm(xo_s, 0)
    tables(1, dev(4))

    def pass_on(kind, r, i=0, links=(1,)):
        wait(kind, r, i)
        for link in links:
            send(kind, r, link, i)

    both = ("wk", "wv")
    for kind in both:
        pass_on(kind, 4, 0, (2, 1))
    pass_on("wq", 4, 0, (2, 1))
    send("wq", 0, 2, 1)
    pass_on("wq", 4, 1, (2, 1))
    for kind in both:
        pass_on(kind, 2)
    for kind in both:
        pass_on(kind, 6)
    wait_shared("wk", 1, 0, wk_s)
    settle(lambda kind, link: link == 1)
    for copy in local[1:3]:
        copy.wait()

    keys_values(0, me)
    for kind in ("k", "v"):
        send(kind, 0, 2)
        send(kind, 0, 1)
    for c in FIRST_Y:
        send("wo", 0, 2, c)
    for c in range(len(WO)):
        send("wo", 0, 1, c)

    def whole_wq(i):
        pass_on("wq", 6, i)
        wait_shared("wq", 1, i, wq_s.at[pl.ds(0, D // 2), pl.ds(i * SGW, SGW)])
        local[3 + i].wait()

    def whole_wq(i):
        pass_on("wq", 6, i)
        wait_shared("wq", 1, i, wq_s.at[pl.ds(0, D // 2), pl.ds(i * SGW, SGW)])
        local[3 + i].wait()

    e = HEAD**-0.5 * LOG2E
    ones = jnp.ones((8, T), jnp.bfloat16)
    per = KH // SG
    pieces = [(kv, n) for kv in range(per) for n in range(G)]
    mine = (me, dev(4))

    def begin():
        top_s[...] = jnp.full(top_s.shape, NEG, jnp.float32)

        def body(n, _):
            mix_s[n // SG, n % SG] = jnp.zeros(mix_s.shape[2:], jnp.float32)

        lax.fori_loop(0, 2 * SG, body, None)

    def step(t, i, j, masked):
        scores = [_dot(k_s[j, i * per + kv], q_s[t, (i * per + kv) * G + n], 1, 1) for kv, n in pieces]
        if masked:
            ok = lax.broadcasted_iota(jnp.int32, (T, T), 0) <= lax.broadcasted_iota(jnp.int32, (T, T), 1)
        weights, keeps = [], []
        for p, s in enumerate(scores):
            if masked:
                s = jnp.where(ok, s, HIDDEN)
            old = top_s[t, i, p : p + 1, :]
            top = jnp.maximum(old, s.max(axis=0, keepdims=True))
            top_s[t, i, p : p + 1, :] = top
            weights.append(jnp.exp2((s - top) * e).astype(jnp.bfloat16))
            keeps.append(jnp.exp2((old - top) * e))
        for p, (kv, n) in enumerate(pieces):
            values = jnp.concatenate([v_s[j, i * per + kv], ones], axis=0)
            mix_s[t, i, p] = mix_s[t, i, p] * keeps[p] + _dot(values, weights[p], 1, 0)

    def last(t):
        return me + t * (dev(4) - me)

    def some(r):
        x, y, k = r // 4, (r // 2) % 2, r % 2
        return 4 * (mx + x - 2 * mx * x) + 2 * (my + y - 2 * my * y) + mk + k - 2 * mk * k

    def over(first, count, item):
        def body(n, _):
            t, i, r = item(n)

            @pl.when(some(r) < last(t))
            def _():
                step(t, i, some(r), False)

        lax.fori_loop(first, count, body, None)

    def diagonal(t):
        lax.fori_loop(0, SG, lambda i, _: step(t, i, mine[t], True), None)

    def finish(t, i, out, base):
        for p in range(len(pieces)):
            total = mix_s[t, i, p, HEAD : HEAD + 1, :]
            at = pl.multiple_of(base + i * SGW + p * HEAD, HEAD)
            out[:, pl.ds(at, HEAD)] = (mix_s[t, i, p, :HEAD, :] * (1 / total)).T.astype(jnp.bfloat16)

    def near():
        begin()
        diagonal(0)
        over(0, SG, lambda n: (0, n, 1))

    def early(first, count):
        over(first, count, lambda n: (1, n // 5, (5 + n % 5) % 6))

    def late(i):
        over(6, 8, lambda n: (1, i, n))
        finish(1, i, give_s, 0)

    def rest(first, count):
        over(first, count, lambda n: (0, n % SG, 2 + n // SG))

    ahead = 2 * SG * mx

    for i in range(SG):
        pass_on("wq", 2, i)
        whole_wq(i)
        queries(0, i)
    wait_shared("k", 1, 0, k_s.at[pl.ds(0, 2)])
    near()
    settle(lambda kind, link: kind in ("wk", "wv", "wq"))
    wait("x", 4)
    norm(xr_s, 1)
    keys_values(1, dev(4))
    for kind in ("k", "v"):
        send(kind, 4, 2)
        send(kind, 4, 1)
    for c in ways("r") + ways("y"):
        if c not in FIRST_Y:
            send("wo", 0, 2, c)
    for kind in ("k", "v"):
        pass_on(kind, 2)
    for c in EARLY_X:
        pass_on("wo", 2, c, (4, 1))
    for i in range(SG):
        queries(1, i)
    wait_shared("k", 3, 0, k_s.at[pl.ds(0, 4)])
    settle(lambda kind, link: link == 1 or kind == "x")
    diagonal(1)
    early(0, 7)
    rest(0, ahead)
    for kind in ("k", "v"):
        pass_on(kind, 6)
    wait_shared("k", 7, 0, k_s.at[pl.ds(0, 2)])
    late(0)
    send("att", 0, 4, 0)
    early(7, 10)
    late(1)
    send("att", 0, 4, 1)
    for c in ways("y", "x"):
        if c not in FIRST_X:
            send("wo", 0, 4, c)
    for c in ways("y"):
        pass_on("wo", 4, c, (2, 1))
    for c in ways("x"):
        if c not in EARLY_X:
            pass_on("wo", 2, c, (4, 1))

    settle(lambda kind, link: kind in ("wk", "wv"))
    half_rows = lambda n, r: pl.ds(pl.multiple_of(n * HALF + (dev(r) - 4 * mx) * ROWS, ROWS), ROWS)

    def half_load(n, r):
        c = ways("r")[n]
        src = wo_ref.at[:, chunk(c)] if r == 0 else place("wo", r, c)
        return pltpu.make_async_copy(src, wk_s.at[half_rows(n, r), :], tile_sem.at[c])

    def half_sum(rows, n, m):
        w = wk_s[pl.ds(n * HALF, HALF), pl.ds(pl.multiple_of(m * 256, 256), 256)]
        return _dot(rows, w, 1, 0)

    for n, c in enumerate(ways("r")):
        pass_on("wo", 2, c)
        wait_shared("wo", 1, c, wof_ref.at[pl.ds(0, 2 * ROWS), chunk(c)])
        for r in range(4):
            half_load(n, r).start()
    for n, c in enumerate(ways("r")):
        whole_tile = wk_s.at[pl.ds(n * HALF, HALF), :]
        pltpu.make_async_copy(whole_tile, whole_tile, tile_sem.at[c]).wait()

        def body(m, _):
            part_s[n, :, pl.ds(pl.multiple_of(m * 256, 256), 256)] = half_sum(give_s[...], n, m).astype(jnp.bfloat16)

        lax.fori_loop(0, WO[c][1] // 256, body, None)
        send("sum", 0, 4, c)

    rest(ahead, 6 * SG)
    for i in range(SG):
        finish(0, i, att_s, mx * HALF)

    for n, c in enumerate(ways("r")):

        def body(m, _):
            mine = att_s[:, pl.ds(pl.multiple_of(mx * HALF, HALF), HALF)]
            sum_s[n, :, pl.ds(pl.multiple_of(m * 256, 256), 256)] = half_sum(mine, n, m)

        lax.fori_loop(0, WO[c][1] // 256, body, None)

    for c in ways("x"):
        if c in FIRST_X:
            pass_on("wo", 4, c)
    for c in ways("y"):
        pass_on("wo", 2, c)
    settle(lambda kind, link: link == 1 or kind in ("wq", "x", "k", "v"))

    def tile(c):
        kind, at = TILES[c]
        return {"wq": wq_s, "wk": wk_s, "wv": wv_s}[kind], at

    def load(c, r):
        ref, at = tile(c)
        src = wo_ref.at[:, chunk(c)] if r == 0 else place("wo", r, c)
        return pltpu.make_async_copy(src, ref.at[wrows(r), pl.ds(at, WO[c][1])], tile_sem.at[c])

    def fetch(c):
        wait_shared("wo", 1, c, wof_ref.at[pl.ds(0, 3 * ROWS), chunk(c)])
        for r in range(6):
            load(c, r).start()

    def write(n):
        c = ORDER[n]
        return pltpu.make_async_copy(out_s.at[n % 2, :, pl.ds(0, WO[c][1])], y_ref.at[:, chunk(c)], out_sem.at[n % 2])

    def project(n, c):
        parts = 512 // WO[c][1]
        size = T // parts

        def body(m, _):
            rows = pl.ds(pl.multiple_of(m % parts * size, size), size)
            at = m // parts * 256
            cols = pl.ds(pl.multiple_of(at, 256), 256)
            if WO[c][2] == "r":
                i = ways("r").index(c)
                y = sum_s[i, rows, cols] + came_s[i, rows, cols].astype(jnp.float32)
            else:
                ref, left = tile(c)
                y = _dot(att_s[rows, :], ref[:, pl.ds(pl.multiple_of(left + at, 256), 256)], 1, 0)
            x = xo_s[rows, pl.ds(pl.multiple_of(WO[c][0] + at, 256), 256)].astype(jnp.float32)
            out_s[n % 2, rows, cols] = (x + y).astype(jnp.bfloat16)

        lax.fori_loop(0, 2, body, None)

    def complete(c):
        pass_on("wo", 6, c)
        if c != FINAL:
            load(c, 6).start()

    far = (2 - 2 * mx) + (1 - my)
    FAR = 2 * ROWS

    def most():
        ref, left = tile(FINAL)
        start, width, _ = WO[FINAL]
        got = ref.at[pl.ds(0, D - FAR), pl.ds(left, width)]
        pltpu.make_async_copy(got, got, tile_sem.at[FINAL]).wait()

        def body(m, _):
            rows = pl.ds(pl.multiple_of(m * 256, 256), 256)
            y = xo_s[rows, pl.ds(start, width)].astype(jnp.float32)
            for n in range(1, 4):
                at = pl.ds(pl.multiple_of((far + n) % 4 * FAR, FAR), FAR)
                y += _dot(att_s[rows, at], ref[at, pl.ds(left, width)], 1, 0)
            most_s[rows, :] = y

        lax.fori_loop(0, T // 256, body, None)
        for copy in kept:
            copy.start()

    kept = [
        pltpu.make_async_copy(most_s, most_ref, local_sem.at[0]),
        pltpu.make_async_copy(att_s.at[:, pl.ds(pl.multiple_of(far * FAR, FAR), FAR)], far_ref, local_sem.at[1]),
    ]

    whole = tuple(c for c in ORDER + (FINAL,) if WO[c][2] != "r")
    after = {c: d for d in whole for c in whole if whole.index(c) < whole.index(d) and TILES[c] == TILES[d]}
    for c in whole:
        if c not in after.values():
            fetch(c)
    for i in range(SG):
        wait("att", 4, i)
    for what, c in STEPS:
        n = ORDER.index(c) if c in ORDER else None
        if what == "pass":
            complete(c)
        elif what == "most":
            most()
        elif what == "load":
            wait("wo", 7, c)
            load(c, 7).start()
        else:
            if WO[c][2] == "r":
                wait("sum", 4, c)
            else:
                ref, at = tile(c)
                whole_tile = ref.at[:, pl.ds(at, WO[c][1])]
                pltpu.make_async_copy(whole_tile, whole_tile, tile_sem.at[c]).wait()
            if n >= 2:
                write(n - 2).wait()
            project(n, c)
            write(n).start()
            if c in after:
                fetch(after[c])
    wait("wo", 7, FINAL)
    for copy in kept:
        copy.wait()
    for n in (len(ORDER) - 2, len(ORDER) - 1):
        write(n).wait()
    settle(lambda kind, link: True)


def _end(part_ref, most_ref, far_ref, wof_ref, y_ref, y_s, most_s, far_s, w_s, in_sem, out_sem):
    me = lax.axis_index("sp")
    start, width, _ = WO[FINAL]
    cols = pl.ds(start, width)
    rows = pl.ds(pl.multiple_of(((2 - me // 4 * 2) + (1 - me // 2 % 2)) * 2 * ROWS, 2 * ROWS), 2 * ROWS)
    first = [
        pltpu.make_async_copy(wof_ref.at[rows, cols], w_s, in_sem.at[PARTS]),
        pltpu.make_async_copy(far_ref, far_s, in_sem.at[PARTS + 1]),
        pltpu.make_async_copy(most_ref, most_s, in_sem.at[PARTS + 2]),
    ]
    size = 2 * T // PARTS
    ways = [(pl.ds(n // 2 * size, size), (pl.ds(0, start), pl.ds(start + width, D - start - width))[n % 2]) for n in range(PARTS)]
    ins = [pltpu.make_async_copy(part_ref.at[at], y_s.at[at], in_sem.at[n]) for n, at in enumerate(ways)]
    outs = [pltpu.make_async_copy(y_s.at[at], y_ref.at[at], out_sem.at[n]) for n, at in enumerate(ways + [(slice(None), cols)])]
    for copy in first + ins:
        copy.start()
    for copy in first:
        copy.wait()
    for n in range(PARTS):
        ins[n].wait()
        outs[n].start()
    y_s[:, cols] = (most_s[...] + _dot(far_s[...], w_s[...], 1, 0)).astype(jnp.bfloat16)
    outs[PARTS].start()
    for copy in outs:
        copy.wait()


PARTS = 8
RS = sum(way == "r" for _, _, way in WO)
SENDS = 42
RECVS = 61


def solution(mesh):
    freq = (THETA ** (-np.arange(HEAD // 2, dtype=np.float32) / (HEAD // 2))).astype(np.float32)
    freq = np.concatenate([freq, freq])[None]
    low = jnp.bfloat16
    vmem = pl.BlockSpec(memory_space=pltpu.VMEM)
    hbm = pl.BlockSpec(memory_space=pl.ANY)

    def step(x, gain, wq, wk, wv, wo):
        part, gathered, most, far = pl.pallas_call(
            _kernel,
            name="half_layer",
            in_specs=[hbm, vmem, vmem, hbm, hbm, hbm, hbm],
            out_specs=[hbm] * 4,
            out_shape=[
                jax.ShapeDtypeStruct((T, D), low),
                jax.ShapeDtypeStruct((D, D), low),
                jax.ShapeDtypeStruct((T, WO[FINAL][1]), jnp.float32),
                jax.ShapeDtypeStruct((T, 2 * ROWS), low),
            ],
            scratch_shapes=[
                pltpu.VMEM((2, T, D), low),
                pltpu.VMEM((T, D), low),
                pltpu.VMEM((T, D), low),
                pltpu.VMEM((D, HALF), low),
                pltpu.VMEM((D, KW), low),
                pltpu.VMEM((D, KW), low),
                pltpu.VMEM((DEVICES, KH, T, HEAD), low),
                pltpu.VMEM((DEVICES, KH, HEAD, T), low),
                pltpu.VMEM((2, KH * G, T, HEAD), low),
                pltpu.VMEM((T, D), low),
                pltpu.VMEM((T, HALF), low),
                pltpu.VMEM((2, T, HEAD), jnp.float32),
                pltpu.VMEM((2, T, HEAD), jnp.float32),
                pltpu.VMEM((2, SG, 8, T), jnp.float32),
                pltpu.VMEM((2, SG, KH // SG * G, HEAD + 8, T), jnp.float32),
                pltpu.VMEM((2, T, 512), low),
                pltpu.VMEM((max(RS, 1), T, 512), jnp.float32),
                pltpu.VMEM((max(RS, 1), T, 512), low),
                pltpu.VMEM((max(RS, 1), T, 512), low),
                pltpu.VMEM((T, WO[FINAL][1]), jnp.float32),
                pltpu.SemaphoreType.DMA((SENDS,)),
                pltpu.SemaphoreType.DMA((RECVS,)),
                pltpu.SemaphoreType.DMA((5,)),
                pltpu.SemaphoreType.DMA((len(WO),)),
                pltpu.SemaphoreType.DMA((2,)),
            ],
            compiler_params=pltpu.CompilerParams(collective_id=0, has_side_effects=True, vmem_limit_bytes=67_000_000),
        )(x, gain, jnp.asarray(freq), wq, wk, wv, wo)
        return pl.pallas_call(
            _end,
            name="end",
            in_specs=[hbm] * 4,
            out_specs=hbm,
            out_shape=jax.ShapeDtypeStruct((T, D), low),
            scratch_shapes=[
                pltpu.VMEM((T, D), low),
                pltpu.VMEM((T, WO[FINAL][1]), jnp.float32),
                pltpu.VMEM((T, 2 * ROWS), low),
                pltpu.VMEM((2 * ROWS, WO[FINAL][1]), low),
                pltpu.SemaphoreType.DMA((PARTS + 3,)),
                pltpu.SemaphoreType.DMA((PARTS + 1,)),
            ],
        )(part, most, far, gathered)

    tokens, whole = P(("dp", "sp"), None), P("sp", None)
    return jax.shard_map(
        step,
        mesh=mesh,
        in_specs=(tokens, P(None), whole, whole, whole, whole),
        out_specs=tokens,
        check_vma=False,
    )
```

```python
import jax
import jax.numpy as jnp
import numpy as np
from jax import lax
from jax.experimental import pallas as pl
from jax.experimental.pallas import tpu as pltpu
from jax.sharding import PartitionSpec as P

HEAD = 128
THETA = 10000
NEG = -1e30
HIDDEN = 2 * NEG
LOG2E = 1.4426950408889634
MESH = pl.DeviceIdType.MESH
DEVICES = 8

T = 512
D = 3072
ROWS = D // DEVICES
HALF = D // 2
KH = 4
KW = KH * HEAD
G = 3
SG = 2
SGW = HALF // SG
WIDTHS = ((512, "y"), (512, "y"), (256, "y"), (256, "y"), (256, "x"), (256, "x"), (512, "r"), (512, "r"))
WO = tuple((sum(w for w, _ in WIDTHS[:n]), *chunk) for n, chunk in enumerate(WIDTHS))
TILES = {0: ("wq", 0), 1: ("wq", 512), 4: ("wq", 1024), 5: ("wq", 1280), 2: ("wv", 0), 3: ("wv", 256)}
EARLY_X = (4, 5)
FINAL = 3
FIRST_X = tuple(range(6))
FIRST_Y = (4, 5, 2)
STEPS = (("pass", 4), ("pass", 5), ("load", 4), ("load", 5), ("done", 4), ("done", 5), ("most", 3), ("pass", 0), ("load", 0), ("done", 0), ("pass", 1), ("load", 1), ("done", 6), ("done", 1), ("pass", 2), ("load", 2), ("pass", 3), ("done", 2), ("done", 7))
ORDER = tuple(c for what, c in STEPS if what == "done")


def _dot(a, b, ca, cb):
    return lax.dot_general(a, b, (((ca,), (cb,)), ((), ())), preferred_element_type=jnp.float32)


def _kernel(
    x_ref, gain_ref, freq_ref, wq_ref, wk_ref, wv_ref, wo_ref,
    y_ref, wof_ref, most_ref, far_ref,
    a_s, xo_s, xr_s, wq_s, wk_s, wv_s, k_s, v_s, q_s, att_s, give_s, cos_s, sin_s, top_s, mix_s, out_s, sum_s, part_s, came_s, most_s,
    send_sem, recv_sem, local_sem, tile_sem, out_sem,
):
    me = lax.axis_index("sp")
    mx, my, mk = me // 4, (me // 2) % 2, me % 2

    def dev(r):
        x = 1 - mx if r & 4 else mx
        y = 1 - my if r & 2 else my
        k = 1 - mk if r & 1 else mk
        return 4 * x + 2 * y + k

    def wrows(r):
        return pl.ds(pl.multiple_of(dev(r) * ROWS, ROWS), ROWS)

    def half(h, width):
        return pl.ds(pl.multiple_of(h * width, width), width)

    def chunk(c):
        return pl.ds(WO[c][0], WO[c][1])

    def ways(*which):
        return tuple(c for c in range(len(WO)) if WO[c][2] in which)

    def place(kind, r, i):
        if kind == "wk":
            return wk_s.at[wrows(r)]
        if kind == "wv":
            return wv_s.at[wrows(r)]
        if kind == "wq":
            return wq_s.at[wrows(r), pl.ds(i * SGW, SGW)]
        if kind == "k":
            return k_s.at[dev(r)]
        if kind == "v":
            return v_s.at[dev(r)]
        if kind == "wo":
            return wof_ref.at[wrows(r), chunk(i)]
        if kind == "x":
            return xr_s
        if kind == "att":
            return give_s.at[:, pl.ds(i * SGW, SGW)]
        if kind == "sum":
            return part_s.at[ways("r").index(i)]

    def own(kind, h, i):
        if kind == "wk":
            return wk_ref.at[:, half(h, KW)]
        if kind == "wv":
            return wv_ref.at[:, half(h, KW)]
        if kind == "wq":
            return wq_ref.at[:, pl.ds(pl.multiple_of(h * HALF + i * SGW, SGW), SGW)]
        if kind == "wo":
            return wo_ref.at[:, chunk(i)]
        if kind == "x":
            return x_ref
        return place(kind, 0, i)

    recv_index = {}

    def recv(kind, r, i):
        key = (kind, r, i)
        if r % 2 and kind in ("wk", "wv"):
            key = ("w", 1, 0)
        elif r % 2 and kind == "wq":
            key = ("wq", 1, i)
        elif r % 2 and kind in ("k", "v"):
            key = ("kv", 3 if r == 5 else r, 0)
        elif r in (1, 3, 5) and kind == "wo":
            key = ("wo", 1, i)
        return recv_sem.at[recv_index.setdefault(key, len(recv_index))]

    def wait_shared(kind, r, i, like):
        sem = recv(kind, r, i)
        pltpu.make_async_remote_copy(
            src_ref=like, dst_ref=like, send_sem=send_sem.at[0], recv_sem=sem, device_id={"sp": dev(4)}, device_id_type=MESH
        ).wait_recv()

    taken = []
    started, settled, free = [], [], list(range(SENDS))

    def settle(which):
        for n, (kind, link, copy) in enumerate(started):
            if n not in settled and which(kind, link):
                copy.wait_send()
                settled.append(n)
                free.append(taken[n])

    def send(kind, r, link, i=0):
        src = own(kind, 1 - mx if link == 4 else mx, i) if r == 0 else place(kind, r, i)
        if kind == "att":
            dst = att_s.at[:, pl.ds(pl.multiple_of(mx * HALF + i * SGW, SGW), SGW)]
        elif kind == "sum":
            dst = came_s.at[ways("r").index(i)]
        else:
            dst = place(kind, r, i)
        taken.append(free.pop(free.index(min(free))))
        copy = pltpu.make_async_remote_copy(
            src_ref=src, dst_ref=dst, send_sem=send_sem.at[taken[-1]], recv_sem=recv(kind, r ^ link, i),
            device_id={"sp": dev(link)}, device_id_type=MESH,
        )
        copy.start()
        started.append((kind, link, copy))

    def wait(kind, r, i=0):
        if kind == "att":
            dst = att_s.at[:, pl.ds(pl.multiple_of((1 - mx) * HALF + i * SGW, SGW), SGW)]
        elif kind == "sum":
            dst = came_s.at[ways("r").index(i)]
        else:
            dst = place(kind, r, i)
        pltpu.make_async_remote_copy(
            src_ref=dst, dst_ref=dst, send_sem=send_sem.at[0], recv_sem=recv(kind, r, i),
            device_id={"sp": dev(4)}, device_id_type=MESH,
        ).wait_recv()

    barrier = pltpu.get_barrier_semaphore()
    for link in (1, 2, 4):
        pl.semaphore_signal(barrier, 1, device_id={"sp": dev(link)}, device_id_type=MESH)
    pl.semaphore_wait(barrier, 3)

    for kind in ("wk", "wv"):
        send(kind, 0, 4)
        send(kind, 0, 2)
    for i in range(SG):
        send("wq", 0, 4, i)
    send("wq", 0, 2, 0)
    send("x", 0, 4)
    for c in FIRST_X:
        send("wo", 0, 4, c)
    local = [
        pltpu.make_async_copy(x_ref, xo_s, local_sem.at[0]),
        pltpu.make_async_copy(own("wk", mx, 0), place("wk", 0, 0), local_sem.at[1]),
        pltpu.make_async_copy(own("wv", mx, 0), place("wv", 0, 0), local_sem.at[2]),
        pltpu.make_async_copy(own("wq", mx, 0), place("wq", 0, 0), local_sem.at[3]),
        pltpu.make_async_copy(own("wq", mx, 1), place("wq", 0, 1), local_sem.at[4]),
    ]
    for copy in local:
        copy.start()
    for kind in ("wk", "wv"):
        send(kind, 0, 1)
    for i in range(SG):
        send("wq", 0, 1, i)

    def tables(t, block):
        def body(i, _):
            at = pl.ds(pl.multiple_of(i * 64, 64), 64)
            token = block * T + i * 64 + lax.broadcasted_iota(jnp.int32, (64, HEAD), 0)
            angle = token.astype(jnp.float32) * freq_ref[...]
            cos_s[t, at, :] = jnp.cos(angle)
            sin = jnp.sin(angle)
            lane = lax.broadcasted_iota(jnp.int32, (64, HEAD), 1)
            sin_s[t, at, :] = jnp.where(lane < HEAD // 2, -sin, sin)

        lax.fori_loop(0, T // 64, body, None)

    def norm(src, t):
        def body(i, _):
            at = pl.ds(pl.multiple_of(i * 32, 32), 32)
            wide = src[at, :].astype(jnp.float32)
            scale = lax.rsqrt(jnp.mean(wide * wide, -1, keepdims=True) + 1e-6)
            a_s[t, at, :] = (wide * scale * gain_ref[...].astype(jnp.float32)[None]).astype(jnp.bfloat16)

        lax.fori_loop(0, T // 32, body, None)

    def turned(t, value):
        wide = value.astype(jnp.bfloat16).astype(jnp.float32)
        return (wide * cos_s[t] + pltpu.roll(wide, HEAD // 2, 1) * sin_s[t]).astype(jnp.bfloat16)

    def keys_values(t, block):
        def body(n, _):
            cols = pl.ds(pl.multiple_of(n * 256, 256), 256)
            k = _dot(a_s[t], wk_s[:, cols], 1, 0)
            v = _dot(a_s[t], wv_s[:, cols], 1, 0).astype(jnp.bfloat16)
            for h in range(2):
                lanes = slice(h * HEAD, (h + 1) * HEAD)
                k_s[block, 2 * n + h] = turned(t, k[:, lanes])
                v_s[block, 2 * n + h] = v[:, lanes].T

        lax.fori_loop(0, KW // 256, body, None)

    def queries(t, i):
        def body(n, _):
            cols = pl.ds(pl.multiple_of(i * SGW + n * 256, 256), 256)
            q = _dot(a_s[t], wq_s[:, cols], 1, 0)
            for h in range(2):
                q_s[t, i * (SGW // HEAD) + 2 * n + h] = turned(t, q[:, h * HEAD : (h + 1) * HEAD])

        lax.fori_loop(0, SGW // 256, body, None)

    local[0].wait()
    tables(0, me)
    norm(xo_s, 0)
    tables(1, dev(4))

    def pass_on(kind, r, i=0, links=(1,)):
        wait(kind, r, i)
        for link in links:
            send(kind, r, link, i)

    both = ("wk", "wv")
    for kind in both:
        pass_on(kind, 4, 0, (2, 1))
    pass_on("wq", 4, 0, (2, 1))
    send("wq", 0, 2, 1)
    pass_on("wq", 4, 1, (2, 1))
    for kind in both:
        pass_on(kind, 2)
    for kind in both:
        pass_on(kind, 6)
    wait_shared("wk", 1, 0, wk_s)
    settle(lambda kind, link: link == 1)
    for copy in local[1:3]:
        copy.wait()

    keys_values(0, me)
    for kind in ("k", "v"):
        send(kind, 0, 2)
        send(kind, 0, 1)
    for c in FIRST_Y:
        send("wo", 0, 2, c)
    for c in range(len(WO)):
        send("wo", 0, 1, c)

    def whole_wq(i):
        pass_on("wq", 6, i)
        wait_shared("wq", 1, i, wq_s.at[pl.ds(0, D // 2), pl.ds(i * SGW, SGW)])
        local[3 + i].wait()

    def whole_wq(i):
        pass_on("wq", 6, i)
        wait_shared("wq", 1, i, wq_s.at[pl.ds(0, D // 2), pl.ds(i * SGW, SGW)])
        local[3 + i].wait()

    e = HEAD**-0.5 * LOG2E
    ones = jnp.ones((8, T), jnp.bfloat16)
    per = KH // SG
    pieces = [(kv, n) for kv in range(per) for n in range(G)]
    mine = (me, dev(4))

    def begin():
        top_s[...] = jnp.full(top_s.shape, NEG, jnp.float32)

        def body(n, _):
            mix_s[n // SG, n % SG] = jnp.zeros(mix_s.shape[2:], jnp.float32)

        lax.fori_loop(0, 2 * SG, body, None)

    def step(t, i, j, masked):
        scores = [_dot(k_s[j, i * per + kv], q_s[t, (i * per + kv) * G + n], 1, 1) for kv, n in pieces]
        if masked:
            ok = lax.broadcasted_iota(jnp.int32, (T, T), 0) <= lax.broadcasted_iota(jnp.int32, (T, T), 1)
        weights, keeps = [], []
        for p, s in enumerate(scores):
            if masked:
                s = jnp.where(ok, s, HIDDEN)
            old = top_s[t, i, p : p + 1, :]
            top = jnp.maximum(old, s.max(axis=0, keepdims=True))
            top_s[t, i, p : p + 1, :] = top
            weights.append(jnp.exp2((s - top) * e).astype(jnp.bfloat16))
            keeps.append(jnp.exp2((old - top) * e))
        for p, (kv, n) in enumerate(pieces):
            values = jnp.concatenate([v_s[j, i * per + kv], ones], axis=0)
            mix_s[t, i, p] = mix_s[t, i, p] * keeps[p] + _dot(values, weights[p], 1, 0)

    def last(t):
        return me + t * (dev(4) - me)

    def some(r):
        x, y, k = r // 4, (r // 2) % 2, r % 2
        return 4 * (mx + x - 2 * mx * x) + 2 * (my + y - 2 * my * y) + mk + k - 2 * mk * k

    def over(first, count, item):
        def body(n, _):
            t, i, r = item(n)

            @pl.when(some(r) < last(t))
            def _():
                step(t, i, some(r), False)

        lax.fori_loop(first, count, body, None)

    def diagonal(t):
        lax.fori_loop(0, SG, lambda i, _: step(t, i, mine[t], True), None)

    def finish(t, i, out, base):
        for p in range(len(pieces)):
            total = mix_s[t, i, p, HEAD : HEAD + 1, :]
            at = pl.multiple_of(base + i * SGW + p * HEAD, HEAD)
            out[:, pl.ds(at, HEAD)] = (mix_s[t, i, p, :HEAD, :] * (1 / total)).T.astype(jnp.bfloat16)

    def near():
        begin()
        diagonal(0)
        over(0, SG, lambda n: (0, n, 1))

    def early(first, count):
        over(first, count, lambda n: (1, n // 5, (5 + n % 5) % 6))

    def late(i):
        over(6, 8, lambda n: (1, i, n))
        finish(1, i, give_s, 0)

    def rest(first, count):
        over(first, count, lambda n: (0, n % SG, 2 + n // SG))

    ahead = 2 * SG * mx

    for i in range(SG):
        pass_on("wq", 2, i)
        whole_wq(i)
        queries(0, i)
    wait_shared("k", 1, 0, k_s.at[pl.ds(0, 2)])
    near()
    settle(lambda kind, link: kind in ("wk", "wv", "wq"))
    wait("x", 4)
    norm(xr_s, 1)
    keys_values(1, dev(4))
    for kind in ("k", "v"):
        send(kind, 4, 2)
        send(kind, 4, 1)
    for c in ways("r") + ways("y"):
        if c not in FIRST_Y:
            send("wo", 0, 2, c)
    for kind in ("k", "v"):
        pass_on(kind, 2)
    for c in EARLY_X:
        pass_on("wo", 2, c, (4, 1))
    for i in range(SG):
        queries(1, i)
    wait_shared("k", 3, 0, k_s.at[pl.ds(0, 4)])
    settle(lambda kind, link: link == 1 or kind == "x")
    diagonal(1)
    early(0, 7)
    rest(0, ahead)
    for kind in ("k", "v"):
        pass_on(kind, 6)
    wait_shared("k", 7, 0, k_s.at[pl.ds(0, 2)])
    late(0)
    send("att", 0, 4, 0)
    early(7, 10)
    late(1)
    send("att", 0, 4, 1)
    for c in ways("y", "x"):
        if c not in FIRST_X:
            send("wo", 0, 4, c)
    for c in ways("y"):
        pass_on("wo", 4, c, (2, 1))
    for c in ways("x"):
        if c not in EARLY_X:
            pass_on("wo", 2, c, (4, 1))

    settle(lambda kind, link: kind in ("wk", "wv"))
    half_rows = lambda n, r: pl.ds(pl.multiple_of(n * HALF + (dev(r) - 4 * mx) * ROWS, ROWS), ROWS)

    def half_load(n, r):
        c = ways("r")[n]
        src = wo_ref.at[:, chunk(c)] if r == 0 else place("wo", r, c)
        return pltpu.make_async_copy(src, wk_s.at[half_rows(n, r), :], tile_sem.at[c])

    def half_sum(rows, n, m):
        w = wk_s[pl.ds(n * HALF, HALF), pl.ds(pl.multiple_of(m * 256, 256), 256)]
        return _dot(rows, w, 1, 0)

    for n, c in enumerate(ways("r")):
        pass_on("wo", 2, c)
        wait_shared("wo", 1, c, wof_ref.at[pl.ds(0, 2 * ROWS), chunk(c)])
        for r in range(4):
            half_load(n, r).start()
    for n, c in enumerate(ways("r")):
        whole_tile = wk_s.at[pl.ds(n * HALF, HALF), :]
        pltpu.make_async_copy(whole_tile, whole_tile, tile_sem.at[c]).wait()

        def body(m, _):
            part_s[n, :, pl.ds(pl.multiple_of(m * 256, 256), 256)] = half_sum(give_s[...], n, m).astype(jnp.bfloat16)

        lax.fori_loop(0, WO[c][1] // 256, body, None)
        send("sum", 0, 4, c)

    rest(ahead, 6 * SG)
    for i in range(SG):
        finish(0, i, att_s, mx * HALF)

    for n, c in enumerate(ways("r")):

        def body(m, _):
            mine = att_s[:, pl.ds(pl.multiple_of(mx * HALF, HALF), HALF)]
            sum_s[n, :, pl.ds(pl.multiple_of(m * 256, 256), 256)] = half_sum(mine, n, m)

        lax.fori_loop(0, WO[c][1] // 256, body, None)

    for c in ways("x"):
        if c in FIRST_X:
            pass_on("wo", 4, c)
    for c in ways("y"):
        pass_on("wo", 2, c)
    settle(lambda kind, link: link == 1 or kind in ("wq", "x", "k", "v"))

    def tile(c):
        kind, at = TILES[c]
        return {"wq": wq_s, "wk": wk_s, "wv": wv_s}[kind], at

    def load(c, r):
        ref, at = tile(c)
        src = wo_ref.at[:, chunk(c)] if r == 0 else place("wo", r, c)
        return pltpu.make_async_copy(src, ref.at[wrows(r), pl.ds(at, WO[c][1])], tile_sem.at[c])

    def fetch(c):
        wait_shared("wo", 1, c, wof_ref.at[pl.ds(0, 3 * ROWS), chunk(c)])
        for r in range(6):
            load(c, r).start()

    def write(n):
        c = ORDER[n]
        return pltpu.make_async_copy(out_s.at[n % 2, :, pl.ds(0, WO[c][1])], y_ref.at[:, chunk(c)], out_sem.at[n % 2])

    def project(n, c):
        parts = 512 // WO[c][1]
        size = T // parts

        def body(m, _):
            rows = pl.ds(pl.multiple_of(m % parts * size, size), size)
            at = m // parts * 256
            cols = pl.ds(pl.multiple_of(at, 256), 256)
            if WO[c][2] == "r":
                i = ways("r").index(c)
                y = sum_s[i, rows, cols] + came_s[i, rows, cols].astype(jnp.float32)
            else:
                ref, left = tile(c)
                y = _dot(att_s[rows, :], ref[:, pl.ds(pl.multiple_of(left + at, 256), 256)], 1, 0)
            x = xo_s[rows, pl.ds(pl.multiple_of(WO[c][0] + at, 256), 256)].astype(jnp.float32)
            out_s[n % 2, rows, cols] = (x + y).astype(jnp.bfloat16)

        lax.fori_loop(0, 2, body, None)

    def complete(c):
        pass_on("wo", 6, c)
        if c != FINAL:
            load(c, 6).start()

    far = (2 - 2 * mx) + (1 - my)
    FAR = 2 * ROWS

    def most():
        ref, left = tile(FINAL)
        start, width, _ = WO[FINAL]
        got = ref.at[pl.ds(0, D - FAR), pl.ds(left, width)]
        pltpu.make_async_copy(got, got, tile_sem.at[FINAL]).wait()

        def body(m, _):
            rows = pl.ds(pl.multiple_of(m * 256, 256), 256)
            y = xo_s[rows, pl.ds(start, width)].astype(jnp.float32)
            for n in range(1, 4):
                at = pl.ds(pl.multiple_of((far + n) % 4 * FAR, FAR), FAR)
                y += _dot(att_s[rows, at], ref[at, pl.ds(left, width)], 1, 0)
            most_s[rows, :] = y

        lax.fori_loop(0, T // 256, body, None)
        for copy in kept:
            copy.start()

    kept = [
        pltpu.make_async_copy(most_s, most_ref, local_sem.at[0]),
        pltpu.make_async_copy(att_s.at[:, pl.ds(pl.multiple_of(far * FAR, FAR), FAR)], far_ref, local_sem.at[1]),
    ]

    whole = tuple(c for c in ORDER + (FINAL,) if WO[c][2] != "r")
    after = {c: d for d in whole for c in whole if whole.index(c) < whole.index(d) and TILES[c] == TILES[d]}
    for c in whole:
        if c not in after.values():
            fetch(c)
    for i in range(SG):
        wait("att", 4, i)
    for what, c in STEPS:
        n = ORDER.index(c) if c in ORDER else None
        if what == "pass":
            complete(c)
        elif what == "most":
            most()
        elif what == "load":
            wait("wo", 7, c)
            load(c, 7).start()
        else:
            if WO[c][2] == "r":
                wait("sum", 4, c)
            else:
                ref, at = tile(c)
                whole_tile = ref.at[:, pl.ds(at, WO[c][1])]
                pltpu.make_async_copy(whole_tile, whole_tile, tile_sem.at[c]).wait()
            if n >= 2:
                write(n - 2).wait()
            project(n, c)
            write(n).start()
            if c in after:
                fetch(after[c])
    wait("wo", 7, FINAL)
    for copy in kept:
        copy.wait()
    for n in (len(ORDER) - 2, len(ORDER) - 1):
        write(n).wait()
    settle(lambda kind, link: True)


def _end(part_ref, most_ref, far_ref, wof_ref, y_ref, y_s, most_s, far_s, w_s, in_sem, out_sem):
    me = lax.axis_index("sp")
    start, width, _ = WO[FINAL]
    cols = pl.ds(start, width)
    rows = pl.ds(pl.multiple_of(((2 - me // 4 * 2) + (1 - me // 2 % 2)) * 2 * ROWS, 2 * ROWS), 2 * ROWS)
    first = [
        pltpu.make_async_copy(wof_ref.at[rows, cols], w_s, in_sem.at[PARTS]),
        pltpu.make_async_copy(far_ref, far_s, in_sem.at[PARTS + 1]),
        pltpu.make_async_copy(most_ref, most_s, in_sem.at[PARTS + 2]),
    ]
    size = 2 * T // PARTS
    ways = [(pl.ds(n // 2 * size, size), (pl.ds(0, start), pl.ds(start + width, D - start - width))[n % 2]) for n in range(PARTS)]
    ins = [pltpu.make_async_copy(part_ref.at[at], y_s.at[at], in_sem.at[n]) for n, at in enumerate(ways)]
    outs = [pltpu.make_async_copy(y_s.at[at], y_ref.at[at], out_sem.at[n]) for n, at in enumerate(ways + [(slice(None), cols)])]
    for copy in first + ins:
        copy.start()
    for copy in first:
        copy.wait()
    for n in range(PARTS // 2):
        ins[n].wait()
        outs[n].start()
    y_s[:, cols] = (most_s[...] + _dot(far_s[...], w_s[...], 1, 0)).astype(jnp.bfloat16)
    outs[PARTS].start()
    for n in range(PARTS // 2, PARTS):
        ins[n].wait()
        outs[n].start()
    for copy in outs:
        copy.wait()


PARTS = 8
RS = sum(way == "r" for _, _, way in WO)
SENDS = 42
RECVS = 61


def solution(mesh):
    freq = (THETA ** (-np.arange(HEAD // 2, dtype=np.float32) / (HEAD // 2))).astype(np.float32)
    freq = np.concatenate([freq, freq])[None]
    low = jnp.bfloat16
    vmem = pl.BlockSpec(memory_space=pltpu.VMEM)
    hbm = pl.BlockSpec(memory_space=pl.ANY)

    def step(x, gain, wq, wk, wv, wo):
        part, gathered, most, far = pl.pallas_call(
            _kernel,
            name="half_layer",
            in_specs=[hbm, vmem, vmem, hbm, hbm, hbm, hbm],
            out_specs=[hbm] * 4,
            out_shape=[
                jax.ShapeDtypeStruct((T, D), low),
                jax.ShapeDtypeStruct((D, D), low),
                jax.ShapeDtypeStruct((T, WO[FINAL][1]), jnp.float32),
                jax.ShapeDtypeStruct((T, 2 * ROWS), low),
            ],
            scratch_shapes=[
                pltpu.VMEM((2, T, D), low),
                pltpu.VMEM((T, D), low),
                pltpu.VMEM((T, D), low),
                pltpu.VMEM((D, HALF), low),
                pltpu.VMEM((D, KW), low),
                pltpu.VMEM((D, KW), low),
                pltpu.VMEM((DEVICES, KH, T, HEAD), low),
                pltpu.VMEM((DEVICES, KH, HEAD, T), low),
                pltpu.VMEM((2, KH * G, T, HEAD), low),
                pltpu.VMEM((T, D), low),
                pltpu.VMEM((T, HALF), low),
                pltpu.VMEM((2, T, HEAD), jnp.float32),
                pltpu.VMEM((2, T, HEAD), jnp.float32),
                pltpu.VMEM((2, SG, 8, T), jnp.float32),
                pltpu.VMEM((2, SG, KH // SG * G, HEAD + 8, T), jnp.float32),
                pltpu.VMEM((2, T, 512), low),
                pltpu.VMEM((max(RS, 1), T, 512), jnp.float32),
                pltpu.VMEM((max(RS, 1), T, 512), low),
                pltpu.VMEM((max(RS, 1), T, 512), low),
                pltpu.VMEM((T, WO[FINAL][1]), jnp.float32),
                pltpu.SemaphoreType.DMA((SENDS,)),
                pltpu.SemaphoreType.DMA((RECVS,)),
                pltpu.SemaphoreType.DMA((5,)),
                pltpu.SemaphoreType.DMA((len(WO),)),
                pltpu.SemaphoreType.DMA((2,)),
            ],
            compiler_params=pltpu.CompilerParams(collective_id=0, has_side_effects=True, vmem_limit_bytes=67_000_000),
        )(x, gain, jnp.asarray(freq), wq, wk, wv, wo)
        return pl.pallas_call(
            _end,
            name="end",
            in_specs=[hbm] * 4,
            out_specs=hbm,
            out_shape=jax.ShapeDtypeStruct((T, D), low),
            scratch_shapes=[
                pltpu.VMEM((T, D), low),
                pltpu.VMEM((T, WO[FINAL][1]), jnp.float32),
                pltpu.VMEM((T, 2 * ROWS), low),
                pltpu.VMEM((2 * ROWS, WO[FINAL][1]), low),
                pltpu.SemaphoreType.DMA((PARTS + 3,)),
                pltpu.SemaphoreType.DMA((PARTS + 1,)),
            ],
        )(part, most, far, gathered)

    tokens, whole = P(("dp", "sp"), None), P("sp", None)
    return jax.shard_map(
        step,
        mesh=mesh,
        in_specs=(tokens, P(None), whole, whole, whole, whole),
        out_specs=tokens,
        check_vma=False,
    )
```
